256 devices in a mesh: rep: 16 (over y, x), shard: 16 (over z, core).
Axes of the slice: x: 4, y: 4, z: 8, core: 2. Of those that a mesh axis runs over, the one named last changes fastest.
Arguments:
- anchor_attn: float32 [2048, 2048], P('shard')
- anchor_ffn: float32 [2048, 5120], P('shard')
- local_attn: float32 [16, 2048, 2048], P('rep', 'shard'), as said below
- local_ffn: float32 [16, 2048, 5120], P('rep', 'shard'), as said below
Outputs:
- outer_attn: float32 [2048, 2048], P('shard')
- outer_ffn: float32 [2048, 5120], P('shard')
Inputs may be any that keep to these rules, and one draw needn't show every extreme that they name: `local_attn`: every replica's weights differ from the anchor. `local_ffn`: every replica's weights differ from the anchor.
All inputs are finite; a program needn't handle non-finite values.
Results may differ from the reference program's by a relative error of at most 0.0003.
Values sent between devices are 32-bit elements; how exact they have to be, the bound alone decides.
No kernel may reach another device: no remote copies, remote signals or barrier semaphores. Data moves between devices by JAX's collectives and lax.ppermute only.
A program may use at most 64 MiB of HBM per device.

```python
import jax
import jax.numpy as jnp
from jax import lax

D = 2048
FF = 5120
REPS = 16


def make_anchor(key, columns, label):
    return jax.random.normal(jax.random.fold_in(key, label), (D, columns), jnp.float32) * D ** (-0.5)


def scale_set(key, columns, label):
    column_key = jax.random.fold_in(key, label + 20)
    row_key = jax.random.fold_in(key, label + 30)
    column_scale = jnp.exp(jax.random.uniform(column_key, (columns,), jnp.float32, 0.0, jnp.log(10.0)))
    rise = jnp.log(3.0)
    ramp = jnp.exp(rise * jnp.arange(D, dtype=jnp.float32) / D)
    row_scale = ramp * jnp.exp(jax.random.uniform(row_key, (D,), jnp.float32, 0.0, jnp.log(3.3)))
    return (row_scale, column_scale)


def replica_levels(key):
    order = jax.random.permutation(jax.random.fold_in(key, 98), REPS).astype(jnp.float32)
    jitter = jax.random.uniform(jax.random.fold_in(key, 99), (REPS,), jnp.float32, 0.2, 0.8)
    level = (order + jitter) / REPS
    return 0.25 * jnp.exp(jnp.log(16.0) * level)


def make_delta(key, columns, label):
    rows_a, cols_a = scale_set(key, D, 1)
    rows_f, cols_f = scale_set(key, FF, 2)
    expected = jnp.sum(rows_a * rows_a) * jnp.sum(cols_a * cols_a) + jnp.sum(rows_f * rows_f) * jnp.sum(cols_f * cols_f)
    normalizer = 1.0 / jnp.sqrt(expected)
    row_scale, column_scale = (rows_a, cols_a) if label == 1 else (rows_f, cols_f)
    noise_key = jax.random.fold_in(key, label + 10)
    noise = jax.random.normal(noise_key, (REPS, D, columns), jnp.float32)
    replica_scale = replica_levels(key) * normalizer
    return noise * replica_scale[:, None, None] * row_scale[None, :, None] * column_scale[None, None, :]


def draw_anchor_attn(key, part):
    return make_anchor(key, D, 1)


def draw_anchor_ffn(key, part):
    return make_anchor(key, FF, 2)


def draw_local_attn(key, part):
    return make_anchor(key, D, 1)[None] + make_delta(key, D, 1)


def draw_local_ffn(key, part):
    return make_anchor(key, FF, 2)[None] + make_delta(key, FF, 2)


def setup_inputs(seed: int = 0) -> dict:
    streams_of = jax.random.split(jax.random.key(seed), 5)
    return {
        "anchor_attn": draw_anchor_attn(jax.random.fold_in(streams_of[4], 71), 0),
        "anchor_ffn": draw_anchor_ffn(jax.random.fold_in(streams_of[4], 71), 0),
        "local_attn": draw_local_attn(jax.random.fold_in(streams_of[4], 71), 0),
        "local_ffn": draw_local_ffn(jax.random.fold_in(streams_of[4], 71), 0),
    }


def reference(anchor_attn, anchor_ffn, local_attn, local_ffn):

    def squares_of(pair):
        one_attn, one_ffn = pair
        delta_a = one_attn - anchor_attn
        delta_f = one_ffn - anchor_ffn
        return jnp.sum(delta_a * delta_a) + jnp.sum(delta_f * delta_f)
    squares = lax.map(squares_of, (local_attn, local_ffn))
    factor = jnp.minimum(jnp.float32(1.0), 1.0 / jnp.sqrt(squares))

    def accumulate(carry, item):
        total_a, total_f = carry
        one_attn, one_ffn, weight = item
        total_a = total_a + weight * (one_attn - anchor_attn)
        total_f = total_f + weight * (one_ffn - anchor_ffn)
        return ((total_a, total_f), None)
    start = (jnp.zeros_like(anchor_attn), jnp.zeros_like(anchor_ffn))
    (total_a, total_f), _ = lax.scan(accumulate, start, (local_attn, local_ffn, factor))
    return (total_a / REPS, total_f / REPS)
```

```python
import jax
import jax.numpy as jnp
from jax import lax
from jax.sharding import Mesh, PartitionSpec as P

SIDE = 4


def shifted(array, axis, step):
    return lax.ppermute(array, axis, [(i, (i + step) % SIDE) for i in range(SIDE)])


def exchanged(value, axis, mask):
    size = lax.axis_size(axis)
    return lax.ppermute(value, axis, [(i, i ^ mask) for i in range(size)])


def at(blocks, index):
    return lax.dynamic_index_in_dim(blocks, index, 0, keepdims=False)


def scattered(blocks, axis):
    me = lax.axis_index(axis)
    return [shifted(at(blocks, (me + k) % SIDE), axis, k) for k in (1, 2, 3)]


def gathered(block, axis):
    me = lax.axis_index(axis)
    pieces = [block] + [shifted(block, axis, k) for k in (1, 2, 3)]
    out = jnp.zeros((SIDE, *block.shape), block.dtype)
    for k, piece in enumerate(pieces):
        out = lax.dynamic_update_index_in_dim(out, piece, (me - k) % SIDE, 0)
    return out


def blocked(array):
    return array.reshape(SIDE, SIDE, array.shape[0] // (SIDE * SIDE), array.shape[1])


def clip_factor(squares):
    return jnp.minimum(jnp.float32(1.0), 1.0 / jnp.sqrt(squares))


def total_over_shard(partial):
    partial = partial + exchanged(partial, "core", 1)
    for mask in (1, 2, 4):
        partial = partial + exchanged(partial, "z", mask)
    return partial


def shards(anchor_attn, anchor_ffn, local_attn, local_ffn):
    local_attn, local_ffn = local_attn[0], local_ffn[0]
    attn, ffn = local_attn.shape[1], local_ffn.shape[1]
    half = (attn + ffn) // 2
    cut = half - attn
    replicas = SIDE * SIDE
    x, y = lax.axis_index("x"), lax.axis_index("y")

    local_a = blocked(jnp.concatenate([local_attn, local_ffn[:, :cut]], axis=1))
    local_b = blocked(local_ffn[:, cut:])
    raw_a = scattered(local_a, "x")
    raw_b = scattered(local_b, "y")

    delta_attn = local_attn - anchor_attn
    delta_ffn = local_ffn - anchor_ffn
    partial = jnp.sum(delta_attn * delta_attn) + jnp.sum(delta_ffn * delta_ffn)
    partial = jnp.full((1, 128), partial)
    factor = clip_factor(total_over_shard(partial))
    factors_a = [factor] + [shifted(factor, "x", k) for k in (1, 2, 3)]
    factors_b = [factor] + [shifted(factor, "y", k) for k in (1, 2, 3)]

    anchor_a = at(blocked(jnp.concatenate([anchor_attn, anchor_ffn[:, :cut]], axis=1)), x)
    anchor_b = at(blocked(anchor_ffn[:, cut:]), y)

    def weighted(blocks, factors, anchor):
        terms = [f[0, 0] * (b - anchor) for b, f in zip(blocks, factors, strict=True)]
        return (terms[0] + terms[1]) + (terms[2] + terms[3])

    sum_a = weighted([at(local_a, x)] + raw_a, factors_a, anchor_a)
    sum_b = weighted([at(local_b, y)] + raw_b, factors_b, anchor_b)

    parts_a = [at(sum_a, y)] + scattered(sum_a, "y")
    parts_b = [at(sum_b, x)] + scattered(sum_b, "x")
    mean_a = ((parts_a[0] + parts_a[1]) + (parts_a[2] + parts_a[3])) / replicas
    mean_b = ((parts_b[0] + parts_b[1]) + (parts_b[2] + parts_b[3])) / replicas

    full_a = gathered(gathered(mean_a, "y"), "x").reshape(-1, half)
    full_b = gathered(gathered(mean_b, "x"), "y").reshape(-1, half)
    return full_a[:, :attn], jnp.concatenate([full_a[:, attn:], full_b], axis=1)


def solution(mesh):
    grid = Mesh(mesh.devices.reshape(SIDE, SIDE, -1, 2), ("y", "x", "z", "core"))
    rep, shard = ("y", "x"), ("z", "core")
    return jax.shard_map(
        shards,
        mesh=grid,
        in_specs=(P(shard, None), P(shard, None), P(rep, shard, None), P(rep, shard, None)),
        out_specs=(P(shard, None), P(shard, None)),
        check_vma=False,
    )
```

```python
import jax
import jax.numpy as jnp
from jax import lax
from jax.sharding import Mesh, PartitionSpec as P

SIDE = 4
CHIP_PLANE = ("y", "x", "core")


def lines(first):
    def member(y, x, core):
        return (y * SIDE + x) * 2 + core

    def along_x(core):
        return [[member(y, x, core) for x in range(SIDE)] for y in range(SIDE)]

    def along_y(core):
        return [[member(y, x, core) for y in range(SIDE)] for x in range(SIDE)]

    return along_x(0) + along_y(1) if first else along_y(0) + along_x(1)


def swapped(blocks, first):
    return lax.all_to_all(blocks, CHIP_PLANE, 0, 0, tiled=True, axis_index_groups=lines(first))


def joined(block, first):
    return lax.all_gather(block, CHIP_PLANE, axis=0, tiled=True, axis_index_groups=lines(first))


def blocked(array):
    return array.reshape(SIDE, array.shape[0] // SIDE, array.shape[1])


def clip_factor(squares):
    return jnp.minimum(jnp.float32(1.0), 1.0 / jnp.sqrt(squares))


def total_over_shard(partial):
    partial = jnp.sum(lax.all_gather(partial, "z", axis=0, tiled=True), axis=0, keepdims=True)
    return partial + lax.ppermute(partial, "core", [(0, 1), (1, 0)])


def shards(anchor_attn, anchor_ffn, local_attn, local_ffn):
    local_attn, local_ffn = local_attn[0], local_ffn[0]
    replicas = SIDE * SIDE
    mine = jnp.where(lax.axis_index("core") == 0, lax.axis_index("x"), lax.axis_index("y"))

    raw_attn = swapped(blocked(local_attn), True)
    raw_ffn = swapped(blocked(local_ffn), True)

    delta_attn = local_attn - anchor_attn
    delta_ffn = local_ffn - anchor_ffn
    partial = jnp.sum(delta_attn * delta_attn) + jnp.sum(delta_ffn * delta_ffn)
    factor = clip_factor(total_over_shard(jnp.full((1, 128), partial)))
    factors = joined(factor, True)[:, :1, None]

    def weighted(raw, anchor):
        anchor = lax.dynamic_index_in_dim(blocked(anchor), mine, 0)
        return jnp.sum(factors * (raw - anchor), axis=0)

    sums = jnp.concatenate([weighted(raw_attn, anchor_attn), weighted(raw_ffn, anchor_ffn)], axis=1)
    mean = jnp.sum(swapped(blocked(sums), False), axis=0) / replicas
    rows = joined(mean, False)

    def spread(block):
        full = swapped(jnp.broadcast_to(block[None], (SIDE, *block.shape)), True)
        return full.reshape(-1, block.shape[1])

    attn = local_attn.shape[1]
    return spread(rows[:, :attn]), spread(rows[:, attn:])


def solution(mesh):
    grid = Mesh(mesh.devices.reshape(SIDE, SIDE, -1, 2), ("y", "x", "z", "core"))
    rep, shard = ("y", "x"), ("z", "core")
    return jax.shard_map(
        shards,
        mesh=grid,
        in_specs=(P(shard, None), P(shard, None), P(rep, shard, None), P(rep, shard, None)),
        out_specs=(P(shard, None), P(shard, None)),
        check_vma=False,
    )
```

```python
import jax
import jax.numpy as jnp
from jax import lax
from jax.sharding import Mesh, PartitionSpec as P

SIDE = 4
REP = ("y", "x")


def hops(step):
    return min(step, SIDE - step)


STEPS = sorted(
    ((dy, dx) for dy in range(SIDE) for dx in range(SIDE) if dy or dx),
    key=lambda s: (hops(s[0]) + hops(s[1]), s),
)


def exchanged(value, axis, mask):
    size = lax.axis_size(axis)
    return lax.ppermute(value, axis, [(i, i ^ mask) for i in range(size)])


def shifted(value, dy, dx):
    pairs = [
        (y * SIDE + x, (y + dy) % SIDE * SIDE + (x + dx) % SIDE)
        for y in range(SIDE)
        for x in range(SIDE)
    ]
    return lax.ppermute(value, REP, pairs)


def clip_factor(squares):
    return jnp.minimum(jnp.float32(1.0), 1.0 / jnp.sqrt(squares))


def squares_of_all(partial, rep):
    lane = lax.broadcasted_iota(jnp.int32, (1, 128), 1)
    total = jnp.where(lane == rep, partial, 0.0)
    for axis, mask in (("core", 1), ("z", 1), ("z", 2), ("z", 4), ("x", 1), ("x", 2), ("y", 1), ("y", 2)):
        total = total + exchanged(total, axis, mask)
    return total


def shards(anchor_attn, anchor_ffn, local_attn, local_ffn):
    local_attn, local_ffn = local_attn[0], local_ffn[0]
    attn, ffn = local_attn.shape[1], local_ffn.shape[1]
    replicas = lax.axis_size(REP)
    y, x = lax.axis_index("y"), lax.axis_index("x")
    rep = y * SIDE + x

    def blocked(array):
        return array.reshape(replicas, -1, array.shape[1])

    both = blocked(jnp.concatenate([local_attn, local_ffn], axis=1))
    raw = lax.all_to_all(both, REP, 0, 0, tiled=True)

    delta_attn = local_attn - anchor_attn
    delta_ffn = local_ffn - anchor_ffn
    partial = jnp.sum(delta_attn * delta_attn) + jnp.sum(delta_ffn * delta_ffn)
    factors = clip_factor(squares_of_all(partial, rep))[0, :replicas]

    anchor = jnp.concatenate(
        [lax.dynamic_index_in_dim(blocked(a), rep, 0, keepdims=False) for a in (anchor_attn, anchor_ffn)], axis=1
    )
    mean = jnp.sum(factors[:, None, None] * (raw - anchor), axis=0) / replicas

    outer_attn = jnp.zeros((replicas, mean.shape[0], attn), mean.dtype)
    outer_ffn = jnp.zeros((replicas, mean.shape[0], ffn), mean.dtype)
    for dy, dx in [(0, 0), *STEPS]:
        rows = shifted(mean, dy, dx) if dy or dx else mean
        source = (y - dy) % SIDE * SIDE + (x - dx) % SIDE
        outer_attn = lax.dynamic_update_index_in_dim(outer_attn, rows[:, :attn], source, 0)
        outer_ffn = lax.dynamic_update_index_in_dim(outer_ffn, rows[:, attn:], source, 0)
    return outer_attn.reshape(-1, attn), outer_ffn.reshape(-1, ffn)


def solution(mesh):
    grid = Mesh(mesh.devices.reshape(SIDE, SIDE, -1, 2), ("y", "x", "z", "core"))
    shard = ("z", "core")
    return jax.shard_map(
        shards,
        mesh=grid,
        in_specs=(P(shard, None), P(shard, None), P(REP, shard, None), P(REP, shard, None)),
        out_specs=(P(shard, None), P(shard, None)),
        check_vma=False,
    )
```

```python
import functools

import jax
import jax.numpy as jnp
from jax import lax
from jax.experimental import pallas as pl
from jax.experimental.pallas import tpu as pltpu
from jax.sharding import Mesh, PartitionSpec as P

SIDE = 4
RING = range(SIDE)
VMEM = pl.BlockSpec(memory_space=pltpu.VMEM)
HBM = pl.BlockSpec(memory_space=pltpu.HBM)
PARAMS = pltpu.CompilerParams(vmem_limit_bytes=16 * 2**20)


def shifted(array, axis, step):
    return lax.ppermute(array, axis, [(i, (i + step) % SIDE) for i in RING])


def paired(value, axis, partner):
    return lax.ppermute(value, axis, list(enumerate(partner)))


def scalar_params(flops, moved):
    return pl.CostEstimate(flops=flops, bytes_accessed=moved, transcendentals=0)


def held(arrays, space=pltpu.VMEM):
    return [pltpu.with_memory_space_constraint(a, space) for a in arrays]


def block_rows(axis, step, rows):
    block = lax.rem(lax.axis_index(axis) + (step + SIDE), SIDE)
    return pl.ds(pl.multiple_of(block * rows, rows), rows)


def pack_kernel(cut, rows, attn, anchor_attn, anchor_ffn, local_attn, local_ffn, *refs):
    packed_a, packed_b = refs[:SIDE], refs[SIDE : 2 * SIDE]
    first_a, first_b, total, later_a, later_b, sems = refs[2 * SIDE :]
    base_a = [first_a] + [later_a.at[k] for k in range(SIDE - 1)]
    base_b = [first_b] + [later_b.at[k] for k in range(SIDE - 1)]

    def fill(k):
        at_a, at_b = block_rows("x", k, rows), block_rows("y", k, rows)
        moves = []
        for n, (src_attn, src_ffn, to_a, to_b) in enumerate(
            ((local_attn, local_ffn, packed_a[k], packed_b[k]), (anchor_attn, anchor_ffn, base_a[k], base_b[k]))
        ):
            moves += [
                pltpu.make_async_copy(src_attn.at[at_a, :], to_a.at[:, pl.ds(0, attn)], sems.at[k, n, 0]),
                pltpu.make_async_copy(src_ffn.at[at_a, pl.ds(0, cut)], to_a.at[:, pl.ds(attn, cut)], sems.at[k, n, 1]),
                pltpu.make_async_copy(src_ffn.at[at_b, pl.ds(cut, attn + cut)], to_b, sems.at[k, n, 2]),
            ]
        return moves

    order = (1, 2, 3, 0)
    moves = {k: fill(k) for k in order}
    for k in order:
        for move in moves[k]:
            move.start()
    width = attn + cut
    sums = jnp.zeros((rows, 128), jnp.float32)
    for k in order:
        for move in moves[k]:
            move.wait()
        for local, base in ((packed_a[k], base_a[k]), (packed_b[k], base_b[k])):

            def step(i, acc, local=local, base=base):
                at = pl.ds(pl.multiple_of(i * 128, 128), 128)
                delta = local[:, at] - base[:, at]
                return acc + delta * delta

            sums = lax.fori_loop(0, width // 128, step, sums, unroll=4)
    total[...] = jnp.full(total.shape, jnp.sum(sums))


def pack(anchor_attn, anchor_ffn, local_attn, local_ffn):
    attn, half = local_attn.shape[1], (local_attn.shape[1] + local_ffn.shape[1]) // 2
    rows = local_attn.shape[0] // SIDE
    block = pltpu.VMEM((rows, half), jnp.float32)
    out = pl.pallas_call(
        functools.partial(pack_kernel, half - attn, rows, attn),
        name="pack",
        out_shape=[block] * (2 * SIDE + 2) + [pltpu.VMEM((8, 128), jnp.float32)],
        in_specs=[HBM] * 4,
        out_specs=[VMEM] * (2 * SIDE + 3),
        scratch_shapes=[
            pltpu.VMEM((SIDE - 1, rows, half), jnp.float32),
            pltpu.VMEM((SIDE - 1, rows, half), jnp.float32),
            pltpu.SemaphoreType.DMA((SIDE, 2, 3)),
        ],
        compiler_params=PARAMS,
        cost_estimate=scalar_params(3 * 8 * rows * half, 16 * 4 * rows * half),
    )(*held([anchor_attn, anchor_ffn, local_attn, local_ffn], pltpu.HBM))
    return out[:SIDE], out[SIDE : 2 * SIDE], out[2 * SIDE], out[2 * SIDE + 1], out[2 * SIDE + 2]


def weigh_kernel(*refs):
    blocks, squares, anchor, out = refs[:SIDE], refs[SIDE : 2 * SIDE], refs[2 * SIDE], refs[2 * SIDE + 1]
    weights = [jnp.minimum(jnp.float32(1.0), 1.0 / jnp.sqrt(s[:1, :1])) for s in squares]

    def step(i, carry):
        at = pl.ds(pl.multiple_of(i * 128, 128), 128)
        base = anchor[:, at]
        t = [w * (b[:, at] - base) for w, b in zip(weights, blocks, strict=True)]
        out[:, at] = (t[0] + t[2]) + (t[1] + t[3])
        return carry

    lax.fori_loop(0, out.shape[1] // 128, step, 0, unroll=4)


def weigh(blocks, squares, anchor):
    return pl.pallas_call(
        weigh_kernel,
        name="weigh",
        out_shape=pltpu.VMEM(anchor.shape, anchor.dtype),
        in_specs=[VMEM] * (2 * SIDE + 1),
        out_specs=VMEM,
        compiler_params=PARAMS,
        cost_estimate=scalar_params(11 * anchor.size, 24 * anchor.size),
    )(*held([*blocks, *squares, anchor]))


def mean_kernel(*refs):
    blocks, out = refs[:SIDE], refs[SIDE]

    def step(i, carry):
        at = pl.ds(pl.multiple_of(i * 128, 128), 128)
        t = [b[:, at] for b in blocks]
        out[:, at] = ((t[0] + t[2]) + (t[1] + t[3])) * jnp.float32(1.0 / (SIDE * SIDE))
        return carry

    lax.fori_loop(0, out.shape[1] // 128, step, 0, unroll=4)


def mean(blocks):
    return pl.pallas_call(
        mean_kernel,
        name="mean",
        out_shape=pltpu.VMEM(blocks[0].shape, blocks[0].dtype),
        in_specs=[VMEM] * SIDE,
        out_specs=VMEM,
        compiler_params=PARAMS,
        cost_estimate=scalar_params(4 * blocks[0].size, 20 * blocks[0].size),
    )(*held(blocks))


def place_kernel(cut, rows, attn, *refs):
    blocks_a, blocks_b = refs[:SIDE], refs[SIDE : 2 * SIDE]
    outer_attn, outer_ffn, sems = refs[2 * SIDE :]
    moves = []
    for k in RING:
        at_a, at_b = block_rows("x", -k, rows), block_rows("y", -k, rows)
        moves += [
            pltpu.make_async_copy(blocks_a[k].at[:, pl.ds(0, attn)], outer_attn.at[at_a, :], sems.at[k, 0]),
            pltpu.make_async_copy(blocks_a[k].at[:, pl.ds(attn, cut)], outer_ffn.at[at_a, pl.ds(0, cut)], sems.at[k, 1]),
            pltpu.make_async_copy(blocks_b[k], outer_ffn.at[at_b, pl.ds(cut, attn + cut)], sems.at[k, 2]),
        ]
    for move in moves:
        move.start()
    for move in moves:
        move.wait()


def place(blocks_a, blocks_b, attn):
    rows, half = blocks_a[0].shape
    shapes = [(SIDE * rows, attn), (SIDE * rows, 2 * half - attn)]
    return pl.pallas_call(
        functools.partial(place_kernel, half - attn, rows, attn),
        name="place",
        out_shape=[jax.ShapeDtypeStruct(s, jnp.float32) for s in shapes],
        in_specs=[VMEM] * (2 * SIDE),
        out_specs=[HBM] * 2,
        scratch_shapes=[pltpu.SemaphoreType.DMA((SIDE, 3))],
        compiler_params=PARAMS,
        cost_estimate=scalar_params(0, 16 * SIDE * rows * half),
    )(*held([*blocks_a, *blocks_b]))


def sent(blocks, axis):
    return [blocks[0]] + [shifted(blocks[k], axis, k) for k in (1, 3, 2)]


def in_order(received):
    own, back_1, back_3, back_2 = received
    return [own, back_1, back_2, back_3]


def total_over_shard(value):
    value = value + paired(value, "core", (1, 0))
    for partner in ((1, 0, 3, 2, 5, 4, 7, 6), (2, 3, 0, 1, 6, 7, 4, 5), (6, 7, 4, 5, 2, 3, 0, 1)):
        value = value + paired(value, "z", partner)
    return value


def shards(anchor_attn, anchor_ffn, local_attn, local_ffn):
    attn = anchor_attn.shape[1]
    blocks_a, blocks_b, anchor_a, anchor_b, partial = pack(anchor_attn, anchor_ffn, local_attn[0], local_ffn[0])
    raw_a = in_order(sent(blocks_a, "x"))
    raw_b = in_order(sent(blocks_b, "y"))
    squares = total_over_shard(partial)
    squares_a = in_order(sent([squares] * SIDE, "x"))
    squares_b = in_order(sent([squares] * SIDE, "y"))
    sum_a = weigh(raw_a, squares_a, anchor_a)
    sum_b = weigh(raw_b, squares_b, anchor_b)
    mean_a = mean(in_order(sent([sum_a] * SIDE, "y")))
    mean_b = mean(in_order(sent([sum_b] * SIDE, "x")))
    return tuple(place(in_order(sent([mean_a] * SIDE, "x")), in_order(sent([mean_b] * SIDE, "y")), attn))


def solution(mesh):
    grid = Mesh(mesh.devices.reshape(SIDE, SIDE, -1, 2), ("y", "x", "z", "core"))
    rep, shard = ("y", "x"), ("z", "core")
    return jax.shard_map(
        shards,
        mesh=grid,
        in_specs=(P(shard, None), P(shard, None), P(rep, shard, None), P(rep, shard, None)),
        out_specs=(P(shard, None), P(shard, None)),
        check_vma=False,
    )
```

```python
import functools

import jax
import jax.numpy as jnp
from jax import lax
from jax.experimental import pallas as pl
from jax.experimental.pallas import tpu as pltpu
from jax.sharding import Mesh, PartitionSpec as P


SIDE = 4
RING = range(SIDE)
VMEM = pl.BlockSpec(memory_space=pltpu.VMEM)
HBM = pl.BlockSpec(memory_space=pltpu.HBM)
PARAMS = pltpu.CompilerParams(vmem_limit_bytes=16 * 2**20)


def shifted(array, axis, step):
    return lax.ppermute(array, axis, [(i, (i + step) % SIDE) for i in RING])


def paired(value, axis, partner):
    return lax.ppermute(value, axis, list(enumerate(partner)))


def scalar_params(flops, moved):
    return pl.CostEstimate(flops=flops, bytes_accessed=moved, transcendentals=0)


def held(arrays, space=pltpu.VMEM):
    return [pltpu.with_memory_space_constraint(a, space) for a in arrays]


def block_rows(axis, step, rows):
    block = lax.rem(lax.axis_index(axis) + (step + SIDE), SIDE)
    return pl.ds(pl.multiple_of(block * rows, rows), rows)


def pack_kernel(cut, rows, attn, anchor_attn, anchor_ffn, local_attn, local_ffn, *refs):
    packed_a, packed_b = refs[:SIDE], refs[SIDE : 2 * SIDE]
    first_a, first_b, total, later_a, later_b, sems = refs[2 * SIDE :]
    base_a = [first_a] + [later_a.at[k] for k in range(SIDE - 1)]
    base_b = [first_b] + [later_b.at[k] for k in range(SIDE - 1)]

    def fill(k):
        at_a, at_b = block_rows("x", k, rows), block_rows("y", k, rows)
        moves = []
        for n, (src_attn, src_ffn, to_a, to_b) in enumerate(
            ((local_attn, local_ffn, packed_a[k], packed_b[k]), (anchor_attn, anchor_ffn, base_a[k], base_b[k]))
        ):
            moves += [
                pltpu.make_async_copy(src_attn.at[at_a, :], to_a.at[:, pl.ds(0, attn)], sems.at[k, n, 0]),
                pltpu.make_async_copy(src_ffn.at[at_a, pl.ds(0, cut)], to_a.at[:, pl.ds(attn, cut)], sems.at[k, n, 1]),
                pltpu.make_async_copy(src_ffn.at[at_b, pl.ds(cut, attn + cut)], to_b, sems.at[k, n, 2]),
            ]
        return moves

    order = (1, 2, 3, 0)
    moves = {k: fill(k) for k in order}
    for k in order:
        for move in moves[k]:
            move.start()
    width = attn + cut
    sums = jnp.zeros((rows, 128), jnp.float32)
    for k in order:
        for move in moves[k]:
            move.wait()
        for local, base in ((packed_a[k], base_a[k]), (packed_b[k], base_b[k])):

            def step(i, acc, local=local, base=base):
                at = pl.ds(pl.multiple_of(i * 128, 128), 128)
                delta = local[:, at] - base[:, at]
                return acc + delta * delta

            sums = lax.fori_loop(0, width // 128, step, sums, unroll=4)
    total[...] = jnp.full(total.shape, jnp.sum(sums))


def pack(anchor_attn, anchor_ffn, local_attn, local_ffn):
    attn, half = local_attn.shape[1], (local_attn.shape[1] + local_ffn.shape[1]) // 2
    rows = local_attn.shape[0] // SIDE
    block = pltpu.VMEM((rows, half), jnp.float32)
    out = pl.pallas_call(
        functools.partial(pack_kernel, half - attn, rows, attn),
        name="pack",
        out_shape=[block] * (2 * SIDE + 2) + [pltpu.VMEM((8, 128), jnp.float32)],
        in_specs=[HBM] * 4,
        out_specs=[VMEM] * (2 * SIDE + 3),
        scratch_shapes=[
            pltpu.VMEM((SIDE - 1, rows, half), jnp.float32),
            pltpu.VMEM((SIDE - 1, rows, half), jnp.float32),
            pltpu.SemaphoreType.DMA((SIDE, 2, 3)),
        ],
        compiler_params=PARAMS,
        cost_estimate=scalar_params(3 * 8 * rows * half, 16 * 4 * rows * half),
    )(*held([anchor_attn, anchor_ffn, local_attn, local_ffn], pltpu.HBM))
    return out[:SIDE], out[SIDE : 2 * SIDE], out[2 * SIDE], out[2 * SIDE + 1], out[2 * SIDE + 2]


def weigh_kernel(axis, rows, *refs):
    blocks, squares, anchor, outs = refs[:SIDE], refs[SIDE : 2 * SIDE], refs[2 * SIDE], refs[2 * SIDE + 1 :]
    weights = [jnp.minimum(jnp.float32(1.0), 1.0 / jnp.sqrt(s[:1, :1])) for s in squares]
    for k, out in enumerate(outs):
        at_rows = block_rows(axis, k, rows)

        def step(i, carry, at_rows=at_rows, out=out):
            at = pl.ds(pl.multiple_of(i * 512, 512), 512)
            base = anchor[at_rows, at]
            t = [w * (b[at_rows, at] - base) for w, b in zip(weights, blocks, strict=True)]
            out[:, at] = (t[0] + t[2]) + (t[1] + t[3])
            return carry

        lax.fori_loop(0, out.shape[1] // 512, step, 0)


def weigh(blocks, squares, anchor, axis):
    rows = anchor.shape[0] // SIDE
    return pl.pallas_call(
        functools.partial(weigh_kernel, axis, rows),
        name="weigh",
        out_shape=[pltpu.VMEM((rows, anchor.shape[1]), anchor.dtype)] * SIDE,
        in_specs=[VMEM] * (2 * SIDE + 1),
        out_specs=[VMEM] * SIDE,
        compiler_params=PARAMS,
        cost_estimate=scalar_params(11 * anchor.size, 24 * anchor.size),
    )(*held([*blocks, *squares, anchor]))


def mean_kernel(*refs):
    blocks, out = refs[:SIDE], refs[SIDE]

    def step(i, carry):
        at = pl.ds(pl.multiple_of(i * 512, 512), 512)
        t = [b[:, at] for b in blocks]
        out[:, at] = ((t[0] + t[2]) + (t[1] + t[3])) * jnp.float32(1.0 / (SIDE * SIDE))
        return carry

    lax.fori_loop(0, out.shape[1] // 512, step, 0)


def mean(blocks):
    return pl.pallas_call(
        mean_kernel,
        name="mean",
        out_shape=pltpu.VMEM(blocks[0].shape, blocks[0].dtype),
        in_specs=[VMEM] * SIDE,
        out_specs=VMEM,
        compiler_params=PARAMS,
        cost_estimate=scalar_params(4 * blocks[0].size, 20 * blocks[0].size),
    )(*held(blocks))


def join_kernel(axis, *refs):
    blocks, out = refs[:SIDE], refs[SIDE]
    rows = blocks[0].shape[0]
    for k, block in enumerate(blocks):
        at_rows = block_rows(axis, -k, rows)

        def step(i, carry, at_rows=at_rows, block=block):
            at = pl.ds(pl.multiple_of(i * 512, 512), 512)
            out[at_rows, at] = block[:, at]
            return carry

        lax.fori_loop(0, block.shape[1] // 512, step, 0)


def join(blocks, axis):
    rows, width = blocks[0].shape
    return pl.pallas_call(
        functools.partial(join_kernel, axis),
        name="join",
        out_shape=pltpu.VMEM((SIDE * rows, width), blocks[0].dtype),
        in_specs=[VMEM] * SIDE,
        out_specs=VMEM,
        compiler_params=PARAMS,
        cost_estimate=scalar_params(rows * width, 32 * rows * width),
    )(*held(blocks))


def place_kernel(cut, rows, attn, *refs):
    blocks_a, blocks_b = refs[:SIDE], refs[SIDE : 2 * SIDE]
    outer_attn, outer_ffn, sems = refs[2 * SIDE :]
    moves = []
    for k in RING:
        at_a, at_b = block_rows("x", -k, rows), block_rows("y", -k, rows)
        moves += [
            pltpu.make_async_copy(blocks_a[k].at[:, pl.ds(0, attn)], outer_attn.at[at_a, :], sems.at[k, 0]),
            pltpu.make_async_copy(blocks_a[k].at[:, pl.ds(attn, cut)], outer_ffn.at[at_a, pl.ds(0, cut)], sems.at[k, 1]),
            pltpu.make_async_copy(blocks_b[k], outer_ffn.at[at_b, pl.ds(cut, attn + cut)], sems.at[k, 2]),
        ]
    for move in moves:
        move.start()
    for move in moves:
        move.wait()


def place(blocks_a, blocks_b, attn):
    rows, half = blocks_a[0].shape
    shapes = [(SIDE * rows, attn), (SIDE * rows, 2 * half - attn)]
    return pl.pallas_call(
        functools.partial(place_kernel, half - attn, rows, attn),
        name="place",
        out_shape=[jax.ShapeDtypeStruct(s, jnp.float32) for s in shapes],
        in_specs=[VMEM] * (2 * SIDE),
        out_specs=[HBM] * 2,
        scratch_shapes=[pltpu.SemaphoreType.DMA((SIDE, 3))],
        compiler_params=PARAMS,
        cost_estimate=scalar_params(0, 16 * SIDE * rows * half),
    )(*held([*blocks_a, *blocks_b]))


def sent(blocks, axis):
    received = {0: blocks[0]}
    for k in (1, 3, 2):
        received[k] = shifted(blocks[k], axis, k)
    return [received[k] for k in RING]


def total_over_shard(value):
    pair, near = (1, 0), (1, 0, 3, 2, 5, 4, 7, 6)
    other = paired(value, "core", pair)
    beside = paired(value, "z", near)
    both = [(2 * z + c, 2 * near[z] + pair[c]) for z in range(len(near)) for c in pair]
    across = lax.ppermute(value, ("z", "core"), both)
    value = (value + other) + (beside + across)
    value = value + paired(value, "z", (2, 3, 0, 1, 6, 7, 4, 5))
    return value + paired(value, "z", (6, 7, 4, 5, 2, 3, 0, 1))


def averaged(anchor_attn, anchor_ffn, local_attn, local_ffn):
    attn = anchor_attn.shape[1]
    blocks_a, blocks_b, anchor_a, anchor_b, partial = pack(anchor_attn, anchor_ffn, local_attn[0], local_ffn[0])
    raw_a = sent(blocks_a, "x")
    raw_b = sent(blocks_b, "y")
    squares = [total_over_shard(partial)] * SIDE
    parts_a = weigh(raw_a, sent(squares, "x"), anchor_a, "y")
    parts_b = weigh(raw_b, sent(squares, "y"), anchor_b, "x")
    mean_a = mean(sent(parts_a, "y"))
    mean_b = mean(sent(parts_b, "x"))
    rows_a = join(sent([mean_a] * SIDE, "y"), "y")
    rows_b = join(sent([mean_b] * SIDE, "x"), "x")
    return tuple(place(sent([rows_a] * SIDE, "x"), sent([rows_b] * SIDE, "y"), attn))


def solution(mesh):
    grid = Mesh(mesh.devices.reshape(SIDE, SIDE, -1, 2), ("y", "x", "z", "core"))
    rep, shard = ("y", "x"), ("z", "core")
    return jax.shard_map(
        averaged,
        mesh=grid,
        in_specs=(P(shard, None), P(shard, None), P(rep, shard, None), P(rep, shard, None)),
        out_specs=(P(shard, None), P(shard, None)),
        check_vma=False,
    )
```

```python
import functools

import jax
import jax.numpy as jnp
from jax import lax
from jax.experimental import pallas as pl
from jax.experimental.pallas import tpu as pltpu
from jax.sharding import Mesh, PartitionSpec as P


SIDE = 4
RING = range(SIDE)
VMEM = pl.BlockSpec(memory_space=pltpu.VMEM)
HBM = pl.BlockSpec(memory_space=pltpu.HBM)
PARAMS = pltpu.CompilerParams(vmem_limit_bytes=16 * 2**20)


def shifted(array, axis, step):
    return lax.ppermute(array, axis, [(i, (i + step) % SIDE) for i in RING])


def paired(value, axis, partner):
    return lax.ppermute(value, axis, list(enumerate(partner)))


def cost_of(flops, moved):
    return pl.CostEstimate(flops=flops, bytes_accessed=moved, transcendentals=0)


def held(arrays, space=pltpu.VMEM):
    return [pltpu.with_memory_space_constraint(a, space) for a in arrays]


def block_rows(axis, step, rows):
    block = lax.rem(lax.axis_index(axis) + (step + SIDE), SIDE)
    return pl.ds(pl.multiple_of(block * rows, rows), rows)


def pack_kernel(cut, rows, attn, anchor_attn, anchor_ffn, local_attn, local_ffn, *refs):
    packed_a, packed_b = refs[:SIDE], refs[SIDE : 2 * SIDE]
    first_a, first_b, total, later_a, later_b, sems = refs[2 * SIDE :]
    base_a = [first_a] + [later_a.at[k] for k in range(SIDE - 1)]
    base_b = [first_b] + [later_b.at[k] for k in range(SIDE - 1)]
    left, rest = pl.ds(0, cut), pl.ds(cut, local_ffn.shape[1] - cut)

    def fill(k):
        at_a, at_b = block_rows("x", k, rows), block_rows("y", k, rows)
        moves = []
        for n, (src_attn, src_ffn, to_a, to_b) in enumerate(
            ((local_attn, local_ffn, packed_a[k], packed_b[k]), (anchor_attn, anchor_ffn, base_a[k], base_b[k]))
        ):
            moves += [
                pltpu.make_async_copy(src_attn.at[at_a, :], to_a.at[:, pl.ds(0, attn)], sems.at[k, n, 0]),
                pltpu.make_async_copy(src_ffn.at[at_a, left], to_a.at[:, pl.ds(attn, cut)], sems.at[k, n, 1]),
                pltpu.make_async_copy(src_ffn.at[at_b, rest], to_b, sems.at[k, n, 2]),
            ]
        return moves

    order = (1, 3, 2, 0)
    moves = {k: fill(k) for k in order}
    for k in order:
        for move in moves[k]:
            move.start()
    sums = jnp.zeros((rows, 128), jnp.float32)
    for k in order:
        for move in moves[k]:
            move.wait()
        for local, base in ((packed_a[k], base_a[k]), (packed_b[k], base_b[k])):

            def step(i, acc, local=local, base=base):
                at = pl.ds(pl.multiple_of(i * 128, 128), 128)
                delta = local[:, at] - base[:, at]
                return acc + delta * delta

            sums = lax.fori_loop(0, local.shape[1] // 128, step, sums, unroll=4)
    total[...] = jnp.full(total.shape, jnp.sum(sums))


def pack(anchor_attn, anchor_ffn, local_attn, local_ffn):
    attn, ffn = local_attn.shape[1], local_ffn.shape[1]
    cut = (attn + ffn) // 7 * 4 - attn
    rows = local_attn.shape[0] // SIDE
    wide, narrow = (rows, attn + cut), (rows, ffn - cut)
    shapes = [wide] * SIDE + [narrow] * SIDE + [wide, narrow, (8, 128)]
    size = local_attn.size + local_ffn.size
    out = pl.pallas_call(
        functools.partial(pack_kernel, cut, rows, attn),
        name="pack",
        out_shape=[pltpu.VMEM(shape, jnp.float32) for shape in shapes],
        in_specs=[HBM] * 4,
        out_specs=[VMEM] * len(shapes),
        scratch_shapes=[
            pltpu.VMEM((SIDE - 1, *wide), jnp.float32),
            pltpu.VMEM((SIDE - 1, *narrow), jnp.float32),
            pltpu.SemaphoreType.DMA((SIDE, 2, 3)),
        ],
        compiler_params=PARAMS,
        cost_estimate=cost_of(3 * size, 16 * size),
    )(*held([anchor_attn, anchor_ffn, local_attn, local_ffn], pltpu.HBM))
    return out[:SIDE], out[SIDE : 2 * SIDE], *out[2 * SIDE :]


def weigh_kernel(*refs):
    blocks, squares, (anchor, out) = refs[:SIDE], refs[SIDE : 2 * SIDE], refs[2 * SIDE :]
    weights = [jnp.minimum(jnp.float32(1.0), 1.0 / jnp.sqrt(s[:1, :1])) for s in squares]

    def step(i, carry):
        at = pl.ds(pl.multiple_of(i * 128, 128), 128)
        base = anchor[:, at]
        t = [w * (b[:, at] - base) for w, b in zip(weights, blocks, strict=True)]
        out[:, at] = (t[0] + t[2]) + (t[1] + t[3])
        return carry

    lax.fori_loop(0, out.shape[1] // 128, step, 0, unroll=4)


def weigh(blocks, squares, anchor):
    return pl.pallas_call(
        weigh_kernel,
        name="weigh",
        out_shape=pltpu.VMEM(anchor.shape, anchor.dtype),
        in_specs=[VMEM] * (2 * SIDE + 1),
        out_specs=VMEM,
        compiler_params=PARAMS,
        cost_estimate=cost_of(11 * anchor.size, 24 * anchor.size),
    )(*held([*blocks, *squares, anchor]))


def mean_kernel(*refs):
    blocks, out = refs[:SIDE], refs[SIDE]

    def step(i, carry):
        at = pl.ds(pl.multiple_of(i * 128, 128), 128)
        t = [b[:, at] for b in blocks]
        out[:, at] = ((t[0] + t[2]) + (t[1] + t[3])) * jnp.float32(1.0 / (SIDE * SIDE))
        return carry

    lax.fori_loop(0, out.shape[1] // 128, step, 0, unroll=4)


def mean(blocks):
    return pl.pallas_call(
        mean_kernel,
        name="mean",
        out_shape=pltpu.VMEM(blocks[0].shape, blocks[0].dtype),
        in_specs=[VMEM] * SIDE,
        out_specs=VMEM,
        compiler_params=PARAMS,
        cost_estimate=cost_of(4 * blocks[0].size, 20 * blocks[0].size),
    )(*held(blocks))


def run(moves):
    for move in moves:
        move.start()
    for move in moves:
        move.wait()


def place_a_kernel(cut, rows, attn, *refs):
    blocks, (outer_attn, outer_ffn, sems) = refs[:SIDE], refs[SIDE:]
    moves = []
    for k in RING:
        at = block_rows("x", -k, rows)
        moves += [
            pltpu.make_async_copy(blocks[k].at[:, pl.ds(0, attn)], outer_attn.at[at, :], sems.at[k, 0]),
            pltpu.make_async_copy(blocks[k].at[:, pl.ds(attn, cut)], outer_ffn.at[at, pl.ds(0, cut)], sems.at[k, 1]),
        ]
    run(moves)


def place_b_kernel(cut, rows, *refs):
    blocks, (_, outer_ffn, sems) = refs[:SIDE], refs[SIDE:]
    columns = pl.ds(cut, outer_ffn.shape[1] - cut)
    run([
        pltpu.make_async_copy(blocks[k], outer_ffn.at[block_rows("y", -k, rows), columns], sems.at[k])
        for k in RING
    ])


def place(blocks_a, blocks_b, attn):
    rows, cut = blocks_a[0].shape[0], blocks_a[0].shape[1] - attn
    outer_attn = jax.ShapeDtypeStruct((SIDE * rows, attn), jnp.float32)
    outer_ffn = jax.ShapeDtypeStruct((SIDE * rows, cut + blocks_b[0].shape[1]), jnp.float32)
    placed_attn, placed_ffn = pl.pallas_call(
        functools.partial(place_a_kernel, cut, rows, attn),
        name="place_a",
        out_shape=[outer_attn, outer_ffn],
        in_specs=[VMEM] * SIDE,
        out_specs=[HBM] * 2,
        scratch_shapes=[pltpu.SemaphoreType.DMA((SIDE, 2))],
        compiler_params=PARAMS,
        cost_estimate=cost_of(0, 32 * blocks_a[0].size),
    )(*held(blocks_a))
    placed_ffn = pl.pallas_call(
        functools.partial(place_b_kernel, cut, rows),
        name="place_b",
        out_shape=outer_ffn,
        in_specs=[VMEM] * SIDE + [HBM],
        out_specs=HBM,
        scratch_shapes=[pltpu.SemaphoreType.DMA((SIDE,))],
        input_output_aliases={SIDE: 0},
        compiler_params=PARAMS,
        cost_estimate=cost_of(0, 32 * blocks_b[0].size),
    )(*held(blocks_b), *held([placed_ffn], pltpu.HBM))
    return placed_attn, placed_ffn


def sent(blocks, axis):
    received = {0: blocks[0]}
    for k in (1, 3, 2):
        received[k] = shifted(blocks[k], axis, k)
    return [received[k] for k in RING]


def total_over_shard(value):
    pair, near = (1, 0), (1, 0, 3, 2, 5, 4, 7, 6)
    other = paired(value, "core", pair)
    beside = paired(value, "z", near)
    both = [(2 * z + c, 2 * near[z] + pair[c]) for z in range(len(near)) for c in pair]
    across = lax.ppermute(value, ("z", "core"), both)
    value = (value + other) + (beside + across)
    value = value + paired(value, "z", (2, 3, 0, 1, 6, 7, 4, 5))
    return value + paired(value, "z", (6, 7, 4, 5, 2, 3, 0, 1))


def averaged(anchor_attn, anchor_ffn, local_attn, local_ffn):
    attn = anchor_attn.shape[1]
    blocks_a, blocks_b, anchor_a, anchor_b, partial = pack(anchor_attn, anchor_ffn, local_attn[0], local_ffn[0])
    raw_a = sent(blocks_a, "x")
    raw_b = sent(blocks_b, "y")
    squares = [total_over_shard(partial)] * SIDE
    sum_a = weigh(raw_a, sent(squares, "x"), anchor_a)
    sum_b = weigh(raw_b, sent(squares, "y"), anchor_b)
    rows_a = mean(sent([sum_a] * SIDE, "y"))
    rows_b = mean(sent([sum_b] * SIDE, "x"))
    return place(sent([rows_a] * SIDE, "x"), sent([rows_b] * SIDE, "y"), attn)


def solution(mesh):
    grid = Mesh(mesh.devices.reshape(SIDE, SIDE, -1, 2), ("y", "x", "z", "core"))
    rep, shard = ("y", "x"), ("z", "core")
    return jax.shard_map(
        averaged,
        mesh=grid,
        in_specs=(P(shard, None), P(shard, None), P(rep, shard, None), P(rep, shard, None)),
        out_specs=(P(shard, None), P(shard, None)),
        check_vma=False,
    )
```

```python
import functools

import jax
import jax.numpy as jnp
from jax import lax
from jax.experimental import pallas as pl
from jax.experimental.pallas import tpu as pltpu
from jax.sharding import Mesh, PartitionSpec as P


SIDE = 4
RING = range(SIDE)
VMEM = pl.BlockSpec(memory_space=pltpu.VMEM)
HBM = pl.BlockSpec(memory_space=pltpu.HBM)
PARAMS = pltpu.CompilerParams(vmem_limit_bytes=16 * 2**20)


def shifted(array, axis, step):
    return lax.ppermute(array, axis, [(i, (i + step) % SIDE) for i in RING])


def paired(value, axis, partner):
    return lax.ppermute(value, axis, list(enumerate(partner)))


def cost_of(flops, moved):
    return pl.CostEstimate(flops=flops, bytes_accessed=moved, transcendentals=0)


def held(arrays, space=pltpu.VMEM):
    return [pltpu.with_memory_space_constraint(a, space) for a in arrays]


def block_rows(axis, step, rows):
    block = lax.rem(lax.axis_index(axis) + (step + SIDE), SIDE)
    return pl.ds(pl.multiple_of(block * rows, rows), rows)


def pack_kernel(cut, rows, attn, anchor_attn, anchor_ffn, local_attn, local_ffn, *refs):
    packed_a, packed_b = refs[:SIDE], refs[SIDE : 2 * SIDE]
    first_a, first_b, total, later_a, later_b, sems = refs[2 * SIDE :]
    base_a = [first_a] + [later_a.at[k] for k in range(SIDE - 1)]
    base_b = [first_b] + [later_b.at[k] for k in range(SIDE - 1)]
    left, rest = pl.ds(0, cut), pl.ds(cut, local_ffn.shape[1] - cut)

    def fill(k):
        at_a, at_b = block_rows("x", k, rows), block_rows("y", k, rows)
        moves = []
        for n, (src_attn, src_ffn, to_a, to_b) in enumerate(
            ((local_attn, local_ffn, packed_a[k], packed_b[k]), (anchor_attn, anchor_ffn, base_a[k], base_b[k]))
        ):
            moves += [
                pltpu.make_async_copy(src_attn.at[at_a, :], to_a.at[:, pl.ds(0, attn)], sems.at[k, n, 0]),
                pltpu.make_async_copy(src_ffn.at[at_a, left], to_a.at[:, pl.ds(attn, cut)], sems.at[k, n, 1]),
                pltpu.make_async_copy(src_ffn.at[at_b, rest], to_b, sems.at[k, n, 2]),
            ]
        return moves

    order = (1, 3, 2, 0)
    moves = {k: fill(k) for k in order}
    for k in order:
        for move in moves[k]:
            move.start()
    sums = jnp.zeros((rows, 128), jnp.float32)
    for k in order:
        for move in moves[k]:
            move.wait()
        for local, base in ((packed_a[k], base_a[k]), (packed_b[k], base_b[k])):

            def step(i, acc, local=local, base=base):
                at = pl.ds(pl.multiple_of(i * 128, 128), 128)
                delta = local[:, at] - base[:, at]
                return acc + delta * delta

            sums = lax.fori_loop(0, local.shape[1] // 128, step, sums, unroll=2)
    total[...] = jnp.full(total.shape, jnp.sum(sums))


def pack(anchor_attn, anchor_ffn, local_attn, local_ffn):
    attn, ffn = local_attn.shape[1], local_ffn.shape[1]
    cut = (attn + ffn) // 28 * 13 - attn
    rows = local_attn.shape[0] // SIDE
    wide, narrow = (rows, attn + cut), (rows, ffn - cut)
    shapes = [wide] * SIDE + [narrow] * SIDE + [wide, narrow, (8, 128)]
    size = local_attn.size + local_ffn.size
    out = pl.pallas_call(
        functools.partial(pack_kernel, cut, rows, attn),
        name="pack",
        out_shape=[pltpu.VMEM(shape, jnp.float32) for shape in shapes],
        in_specs=[HBM] * 4,
        out_specs=[VMEM] * len(shapes),
        scratch_shapes=[
            pltpu.VMEM((SIDE - 1, *wide), jnp.float32),
            pltpu.VMEM((SIDE - 1, *narrow), jnp.float32),
            pltpu.SemaphoreType.DMA((SIDE, 2, 3)),
        ],
        compiler_params=PARAMS,
        cost_estimate=cost_of(3 * size, 16 * size),
    )(*held([anchor_attn, anchor_ffn, local_attn, local_ffn], pltpu.HBM))
    return out[:SIDE], out[SIDE : 2 * SIDE], *out[2 * SIDE :]


def weigh_kernel(axis, rows, pieces, *refs):
    blocks, squares, anchor, outs = refs[:SIDE], refs[SIDE : 2 * SIDE], refs[2 * SIDE], refs[-pieces:]
    weights = [jnp.minimum(jnp.float32(1.0), 1.0 / jnp.sqrt(s[:1, :1])) for s in squares]
    for k, out in enumerate(outs):
        at_rows = block_rows(axis, k, rows) if len(outs) > 1 else slice(None)

        def step(i, carry, at_rows=at_rows, out=out):
            at = pl.ds(pl.multiple_of(i * 128, 128), 128)
            base = anchor[at_rows, at]
            t = [w * (b[at_rows, at] - base) for w, b in zip(weights, blocks, strict=True)]
            out[:, at] = (t[0] + t[2]) + (t[1] + t[3])
            return carry

        lax.fori_loop(0, out.shape[1] // 128, step, 0, unroll=2)


def weigh(blocks, squares, anchor, axis, pieces, after=()):
    rows = anchor.shape[0] // pieces
    return pl.pallas_call(
        functools.partial(weigh_kernel, axis, rows, pieces),
        name="weigh",
        out_shape=[pltpu.VMEM((rows, anchor.shape[1]), anchor.dtype)] * pieces,
        in_specs=[VMEM] * (2 * SIDE + 1 + len(after)),
        out_specs=[VMEM] * pieces,
        compiler_params=PARAMS,
        cost_estimate=cost_of(11 * anchor.size, 24 * anchor.size),
    )(*held([*blocks, *squares, anchor, *after]))


def mean_kernel(*refs):
    blocks, out = refs[:SIDE], refs[SIDE]

    def step(i, carry):
        at = pl.ds(pl.multiple_of(i * 128, 128), 128)
        t = [b[:, at] for b in blocks]
        out[:, at] = ((t[0] + t[2]) + (t[1] + t[3])) * jnp.float32(1.0 / (SIDE * SIDE))
        return carry

    lax.fori_loop(0, out.shape[1] // 128, step, 0, unroll=2)


def mean(blocks):
    return pl.pallas_call(
        mean_kernel,
        name="mean",
        out_shape=pltpu.VMEM(blocks[0].shape, blocks[0].dtype),
        in_specs=[VMEM] * SIDE,
        out_specs=VMEM,
        compiler_params=PARAMS,
        cost_estimate=cost_of(4 * blocks[0].size, 20 * blocks[0].size),
    )(*held(blocks))


def join_kernel(axis, *refs):
    blocks, out = refs[:SIDE], refs[SIDE]
    rows = blocks[0].shape[0]
    for k, block in enumerate(blocks):
        at_rows = block_rows(axis, -k, rows)

        def step(i, carry, at_rows=at_rows, block=block):
            at = pl.ds(pl.multiple_of(i * 256, 256), 256)
            out[at_rows, at] = block[:, at]
            return carry

        lax.fori_loop(0, block.shape[1] // 256, step, 0)


def join(blocks, axis):
    rows, width = blocks[0].shape
    return pl.pallas_call(
        functools.partial(join_kernel, axis),
        name="join",
        out_shape=pltpu.VMEM((SIDE * rows, width), blocks[0].dtype),
        in_specs=[VMEM] * SIDE,
        out_specs=VMEM,
        compiler_params=PARAMS,
        cost_estimate=cost_of(rows * width, 32 * rows * width),
    )(*held(blocks))


def run(moves):
    for move in moves:
        move.start()
    for move in moves:
        move.wait()


def place_a_kernel(cut, rows, attn, *refs):
    blocks, (outer_attn, outer_ffn, sems) = refs[:SIDE], refs[SIDE:]
    moves = []
    for k in RING:
        at = block_rows("x", -k, rows)
        moves += [
            pltpu.make_async_copy(blocks[k].at[:, pl.ds(0, attn)], outer_attn.at[at, :], sems.at[k, 0]),
            pltpu.make_async_copy(blocks[k].at[:, pl.ds(attn, cut)], outer_ffn.at[at, pl.ds(0, cut)], sems.at[k, 1]),
        ]
    run(moves)


def place_b_kernel(cut, rows, *refs):
    blocks, (_, outer_ffn, sems) = refs[:SIDE], refs[SIDE:]
    columns = pl.ds(cut, outer_ffn.shape[1] - cut)
    run([
        pltpu.make_async_copy(blocks[k], outer_ffn.at[block_rows("y", -k, rows), columns], sems.at[k])
        for k in RING
    ])


def place(blocks_a, blocks_b, attn):
    rows, cut = blocks_a[0].shape[0], blocks_a[0].shape[1] - attn
    outer_attn = jax.ShapeDtypeStruct((SIDE * rows, attn), jnp.float32)
    outer_ffn = jax.ShapeDtypeStruct((SIDE * rows, cut + blocks_b[0].shape[1]), jnp.float32)
    placed_attn, placed_ffn = pl.pallas_call(
        functools.partial(place_a_kernel, cut, rows, attn),
        name="place_a",
        out_shape=[outer_attn, outer_ffn],
        in_specs=[VMEM] * SIDE,
        out_specs=[HBM] * 2,
        scratch_shapes=[pltpu.SemaphoreType.DMA((SIDE, 2))],
        compiler_params=PARAMS,
        cost_estimate=cost_of(0, 32 * blocks_a[0].size),
    )(*held(blocks_a))
    placed_ffn = pl.pallas_call(
        functools.partial(place_b_kernel, cut, rows),
        name="place_b",
        out_shape=outer_ffn,
        in_specs=[VMEM] * SIDE + [HBM],
        out_specs=HBM,
        scratch_shapes=[pltpu.SemaphoreType.DMA((SIDE,))],
        input_output_aliases={SIDE: 0},
        compiler_params=PARAMS,
        cost_estimate=cost_of(0, 32 * blocks_b[0].size),
    )(*held(blocks_b), *held([placed_ffn], pltpu.HBM))
    return placed_attn, placed_ffn


def sent(blocks, axis):
    received = {0: blocks[0]}
    for k in (1, 3, 2):
        received[k] = shifted(blocks[k], axis, k)
    return [received[k] for k in RING]


def total_over_shard(value):
    pair, near = (1, 0), (1, 0, 3, 2, 5, 4, 7, 6)
    other = paired(value, "core", pair)
    beside = paired(value, "z", near)
    both = [(2 * z + c, 2 * near[z] + pair[c]) for z in range(len(near)) for c in pair]
    across = lax.ppermute(value, ("z", "core"), both)
    value = (value + other) + (beside + across)
    value = value + paired(value, "z", (2, 3, 0, 1, 6, 7, 4, 5))
    return value + paired(value, "z", (6, 7, 4, 5, 2, 3, 0, 1))


def averaged(anchor_attn, anchor_ffn, local_attn, local_ffn):
    attn = anchor_attn.shape[1]
    blocks_a, blocks_b, anchor_a, anchor_b, partial = pack(anchor_attn, anchor_ffn, local_attn[0], local_ffn[0])
    raw_a = sent(blocks_a, "x")
    raw_b = sent(blocks_b, "y")
    squares = [total_over_shard(partial)] * SIDE
    parts_b = weigh(raw_b, sent(squares, "y"), anchor_b, "x", SIDE)
    (sum_a,) = weigh(raw_a, sent(squares, "x"), anchor_a, "y", 1, parts_b[:1])
    mean_b = mean(sent(parts_b, "x"))
    rows_a = mean(sent([sum_a] * SIDE, "y"))
    rows_b = join(sent([mean_b] * SIDE, "x"), "x")
    back_b = sent([rows_b] * SIDE, "y")
    return place(sent([rows_a] * SIDE, "x"), back_b, attn)


def solution(mesh):
    grid = Mesh(mesh.devices.reshape(SIDE, SIDE, -1, 2), ("y", "x", "z", "core"))
    rep, shard = ("y", "x"), ("z", "core")
    return jax.shard_map(
        averaged,
        mesh=grid,
        in_specs=(P(shard, None), P(shard, None), P(rep, shard, None), P(rep, shard, None)),
        out_specs=(P(shard, None), P(shard, None)),
        check_vma=False,
    )
```

```python
import functools

import jax
import jax.numpy as jnp
from jax import lax
from jax.experimental import pallas as pl
from jax.experimental.pallas import tpu as pltpu
from jax.sharding import Mesh, PartitionSpec as P


SIDE = 4
RING = range(SIDE)
VMEM = pl.BlockSpec(memory_space=pltpu.VMEM)
HBM = pl.BlockSpec(memory_space=pltpu.HBM)
PARAMS = pltpu.CompilerParams(vmem_limit_bytes=16 * 2**20)


def shifted(array, axis, step):
    return lax.ppermute(array, axis, [(i, (i + step) % SIDE) for i in RING])


def paired(value, axis, partner):
    return lax.ppermute(value, axis, list(enumerate(partner)))


def cost_of(flops, moved):
    return pl.CostEstimate(flops=flops, bytes_accessed=moved, transcendentals=0)


def held(arrays, space=pltpu.VMEM):
    return [pltpu.with_memory_space_constraint(a, space) for a in arrays]


def block_rows(axis, step, rows):
    block = lax.rem(lax.axis_index(axis) + (step + SIDE), SIDE)
    return pl.ds(pl.multiple_of(block * rows, rows), rows)


def pack_kernel(cut, rows, attn, anchor_attn, anchor_ffn, local_attn, local_ffn, *refs):
    packed_a, packed_b = refs[:SIDE], refs[SIDE : 2 * SIDE]
    first_a, first_b, total, later_a, later_b, sems = refs[2 * SIDE :]
    base_a = [first_a] + [later_a.at[k] for k in range(SIDE - 1)]
    base_b = [first_b] + [later_b.at[k] for k in range(SIDE - 1)]
    left, rest = pl.ds(0, cut), pl.ds(cut, local_ffn.shape[1] - cut)

    def fill(k):
        at_a, at_b = block_rows("x", k, rows), block_rows("y", k, rows)
        moves = []
        for n, (src_attn, src_ffn, to_a, to_b) in enumerate(
            ((local_attn, local_ffn, packed_a[k], packed_b[k]), (anchor_attn, anchor_ffn, base_a[k], base_b[k]))
        ):
            moves += [
                pltpu.make_async_copy(src_attn.at[at_a, :], to_a.at[:, pl.ds(0, attn)], sems.at[k, n, 0]),
                pltpu.make_async_copy(src_ffn.at[at_a, left], to_a.at[:, pl.ds(attn, cut)], sems.at[k, n, 1]),
                pltpu.make_async_copy(src_ffn.at[at_b, rest], to_b, sems.at[k, n, 2]),
            ]
        return moves

    order = (1, 3, 2, 0)
    moves = {k: fill(k) for k in order}
    for k in order:
        for move in moves[k]:
            move.start()
    sums = jnp.zeros((rows, 128), jnp.float32)
    for k in order:
        for move in moves[k]:
            move.wait()
        for local, base in ((packed_a[k], base_a[k]), (packed_b[k], base_b[k])):

            def step(i, acc, local=local, base=base):
                at = pl.ds(pl.multiple_of(i * 128, 128), 128)
                delta = local[:, at] - base[:, at]
                return acc + delta * delta

            sums = lax.fori_loop(0, local.shape[1] // 128, step, sums, unroll=2)
    total[...] = jnp.full(total.shape, jnp.sum(sums))


def pack(anchor_attn, anchor_ffn, local_attn, local_ffn):
    attn, ffn = local_attn.shape[1], local_ffn.shape[1]
    cut = (attn + ffn) // 28 * 13 - attn
    rows = local_attn.shape[0] // SIDE
    wide, narrow = (rows, attn + cut), (rows, ffn - cut)
    shapes = [wide] * SIDE + [narrow] * SIDE + [wide, narrow, (8, 128)]
    size = local_attn.size + local_ffn.size
    out = pl.pallas_call(
        functools.partial(pack_kernel, cut, rows, attn),
        name="pack",
        out_shape=[pltpu.VMEM(shape, jnp.float32) for shape in shapes],
        in_specs=[HBM] * 4,
        out_specs=[VMEM] * len(shapes),
        scratch_shapes=[
            pltpu.VMEM((SIDE - 1, *wide), jnp.float32),
            pltpu.VMEM((SIDE - 1, *narrow), jnp.float32),
            pltpu.SemaphoreType.DMA((SIDE, 2, 3)),
        ],
        compiler_params=PARAMS,
        cost_estimate=cost_of(3 * size, 16 * size),
    )(*held([anchor_attn, anchor_ffn, local_attn, local_ffn], pltpu.HBM))
    return out[:SIDE], out[SIDE : 2 * SIDE], *out[2 * SIDE :]


def weigh_kernel(axis, rows, pieces, *refs):
    blocks, squares, anchor, outs = refs[:SIDE], refs[SIDE], refs[SIDE + 1], refs[-pieces:]
    factors = jnp.minimum(jnp.float32(1.0), 1.0 / jnp.sqrt(squares[...]))
    first = 0 if axis == "y" else SIDE - 1
    weights = [factors[k : k + 1, :1] for k in (0, *range(first + 1, first + SIDE))]
    for k, out in enumerate(outs):
        at_rows = block_rows(axis, k, rows) if len(outs) > 1 else slice(None)

        def step(i, carry, at_rows=at_rows, out=out):
            at = pl.ds(pl.multiple_of(i * 128, 128), 128)
            base = anchor[at_rows, at]
            t = [w * (b[at_rows, at] - base) for w, b in zip(weights, blocks, strict=True)]
            out[:, at] = (t[0] + t[2]) + (t[1] + t[3])
            return carry

        lax.fori_loop(0, out.shape[1] // 128, step, 0, unroll=2 if len(outs) == 1 else 6)


def weigh(blocks, squares, anchor, axis, pieces, after=()):
    rows = anchor.shape[0] // pieces
    return pl.pallas_call(
        functools.partial(weigh_kernel, axis, rows, pieces),
        name="weigh",
        out_shape=[pltpu.VMEM((rows, anchor.shape[1]), anchor.dtype)] * pieces,
        in_specs=[VMEM] * (SIDE + 2 + len(after)),
        out_specs=[VMEM] * pieces,
        compiler_params=PARAMS,
        cost_estimate=cost_of(11 * anchor.size, 24 * anchor.size),
    )(*held([*blocks, squares, anchor, *after]))


def mean_kernel(*refs):
    blocks, out = refs[:SIDE], refs[SIDE]

    def step(i, carry):
        at = pl.ds(pl.multiple_of(i * 128, 128), 128)
        t = [b[:, at] for b in blocks]
        out[:, at] = ((t[0] + t[2]) + (t[1] + t[3])) * jnp.float32(1.0 / (SIDE * SIDE))
        return carry

    lax.fori_loop(0, out.shape[1] // 128, step, 0, unroll=2)


def mean(blocks):
    return pl.pallas_call(
        mean_kernel,
        name="mean",
        out_shape=pltpu.VMEM(blocks[0].shape, blocks[0].dtype),
        in_specs=[VMEM] * SIDE,
        out_specs=VMEM,
        compiler_params=PARAMS,
        cost_estimate=cost_of(4 * blocks[0].size, 20 * blocks[0].size),
    )(*held(blocks))


def join_kernel(axis, *refs):
    blocks, out = refs[:SIDE], refs[SIDE]
    rows = blocks[0].shape[0]
    for k, block in enumerate(blocks):
        at_rows = block_rows(axis, -k, rows)

        def step(i, carry, at_rows=at_rows, block=block):
            at = pl.ds(pl.multiple_of(i * 256, 256), 256)
            out[at_rows, at] = block[:, at]
            return carry

        lax.fori_loop(0, block.shape[1] // 256, step, 0)


def join(blocks, axis):
    rows, width = blocks[0].shape
    return pl.pallas_call(
        functools.partial(join_kernel, axis),
        name="join",
        out_shape=pltpu.VMEM((SIDE * rows, width), blocks[0].dtype),
        in_specs=[VMEM] * SIDE,
        out_specs=VMEM,
        compiler_params=PARAMS,
        cost_estimate=cost_of(rows * width, 32 * rows * width),
    )(*held(blocks))


def run(moves):
    for move in moves:
        move.start()
    for move in moves:
        move.wait()


def place_a_kernel(cut, rows, attn, *refs):
    blocks, (outer_attn, outer_ffn, sems) = refs[:SIDE], refs[SIDE:]
    moves = []
    for k in RING:
        at = block_rows("x", -k, rows)
        moves += [
            pltpu.make_async_copy(blocks[k].at[:, pl.ds(0, attn)], outer_attn.at[at, :], sems.at[k, 0]),
            pltpu.make_async_copy(blocks[k].at[:, pl.ds(attn, cut)], outer_ffn.at[at, pl.ds(0, cut)], sems.at[k, 1]),
        ]
    run(moves)


def place_b_kernel(cut, rows, *refs):
    blocks, (_, outer_ffn, sems) = refs[:SIDE], refs[SIDE:]
    columns = pl.ds(cut, outer_ffn.shape[1] - cut)
    run([
        pltpu.make_async_copy(blocks[k], outer_ffn.at[block_rows("y", -k, rows), columns], sems.at[k])
        for k in RING
    ])


def place(blocks_a, blocks_b, attn):
    rows, cut = blocks_a[0].shape[0], blocks_a[0].shape[1] - attn
    outer_attn = jax.ShapeDtypeStruct((SIDE * rows, attn), jnp.float32)
    outer_ffn = jax.ShapeDtypeStruct((SIDE * rows, cut + blocks_b[0].shape[1]), jnp.float32)
    placed_attn, placed_ffn = pl.pallas_call(
        functools.partial(place_a_kernel, cut, rows, attn),
        name="place_a",
        out_shape=[outer_attn, outer_ffn],
        in_specs=[VMEM] * SIDE,
        out_specs=[HBM] * 2,
        scratch_shapes=[pltpu.SemaphoreType.DMA((SIDE, 2))],
        compiler_params=PARAMS,
        cost_estimate=cost_of(0, 32 * blocks_a[0].size),
    )(*held(blocks_a))
    placed_ffn = pl.pallas_call(
        functools.partial(place_b_kernel, cut, rows),
        name="place_b",
        out_shape=outer_ffn,
        in_specs=[VMEM] * SIDE + [HBM],
        out_specs=HBM,
        scratch_shapes=[pltpu.SemaphoreType.DMA((SIDE,))],
        input_output_aliases={SIDE: 0},
        compiler_params=PARAMS,
        cost_estimate=cost_of(0, 32 * blocks_b[0].size),
    )(*held(blocks_b), *held([placed_ffn], pltpu.HBM))
    return placed_attn, placed_ffn


def sent(blocks, axis):
    received = {0: blocks[0]}
    for k in (1, 3, 2):
        received[k] = shifted(blocks[k], axis, k)
    return [received[k] for k in RING]


def total_over_shard(value):
    pair, near = (1, 0), (1, 0, 3, 2, 5, 4, 7, 6)
    other = paired(value, "core", pair)
    beside = paired(value, "z", near)
    both = [(2 * z + c, 2 * near[z] + pair[c]) for z in range(len(near)) for c in pair]
    across = lax.ppermute(value, ("z", "core"), both)
    value = (value + other) + (beside + across)
    value = value + paired(value, "z", (2, 3, 0, 1, 6, 7, 4, 5))
    return value + paired(value, "z", (6, 7, 4, 5, 2, 3, 0, 1))


def averaged(anchor_attn, anchor_ffn, local_attn, local_ffn):
    attn = anchor_attn.shape[1]
    blocks_a, blocks_b, anchor_a, anchor_b, partial = pack(anchor_attn, anchor_ffn, local_attn[0], local_ffn[0])
    raw_a = sent(blocks_a, "x")
    raw_b = sent(blocks_b, "y")
    ones = [partial] * SIDE
    along_y, along_x = sent(ones, "y"), sent(ones, "x")
    row = lax.broadcasted_iota(jnp.int32, partial.shape, 0)
    lines = partial
    for k, value in enumerate(along_x[1:] + along_y[1:]):
        lines = jnp.where(row == k + 1, value, lines)
    squares = total_over_shard(lines)
    parts_b = weigh(raw_b, squares, anchor_b, "x", SIDE)
    (sum_a,) = weigh(raw_a, squares, anchor_a, "y", 1, parts_b[:1])
    mean_b = mean(sent(parts_b, "x"))
    rows_a = mean(sent([sum_a] * SIDE, "y"))
    rows_b = join(sent([mean_b] * SIDE, "x"), "x")
    back_b = sent([rows_b] * SIDE, "y")
    return place(sent([rows_a] * SIDE, "x"), back_b, attn)


def solution(mesh):
    grid = Mesh(mesh.devices.reshape(SIDE, SIDE, -1, 2), ("y", "x", "z", "core"))
    rep, shard = ("y", "x"), ("z", "core")
    return jax.shard_map(
        averaged,
        mesh=grid,
        in_specs=(P(shard, None), P(shard, None), P(rep, shard, None), P(rep, shard, None)),
        out_specs=(P(shard, None), P(shard, None)),
        check_vma=False,
    )
```

```python
import functools

import jax
import jax.numpy as jnp
from jax import lax
from jax.experimental import pallas as pl
from jax.experimental.pallas import tpu as pltpu
from jax.sharding import Mesh, PartitionSpec as P


SIDE = 4
RING = range(SIDE)
VMEM = pl.BlockSpec(memory_space=pltpu.VMEM)
HBM = pl.BlockSpec(memory_space=pltpu.HBM)
PARAMS = pltpu.CompilerParams(vmem_limit_bytes=16 * 2**20)


def shifted(array, axis, step):
    return lax.ppermute(array, axis, [(i, (i + step) % SIDE) for i in RING])


def paired(value, axis, partner):
    return lax.ppermute(value, axis, list(enumerate(partner)))


def cost_of(flops, moved):
    return pl.CostEstimate(flops=flops, bytes_accessed=moved, transcendentals=0)


def held(arrays, space=pltpu.VMEM):
    return [pltpu.with_memory_space_constraint(a, space) for a in arrays]


def block_rows(axis, step, rows):
    block = lax.rem(lax.axis_index(axis) + (step + SIDE), SIDE)
    return pl.ds(pl.multiple_of(block * rows, rows), rows)


def pack_kernel(cut, rows, attn, anchor_attn, anchor_ffn, local_attn, local_ffn, *refs):
    packed_a, packed_b = refs[:SIDE], refs[SIDE : 2 * SIDE]
    first_a, first_b, total, later_a, later_b, sems = refs[2 * SIDE :]
    base_a = [first_a] + [later_a.at[k] for k in range(SIDE - 1)]
    base_b = [first_b] + [later_b.at[k] for k in range(SIDE - 1)]
    left, rest = pl.ds(0, cut), pl.ds(cut, local_ffn.shape[1] - cut)

    def fill(k):
        at_a, at_b = block_rows("x", k, rows), block_rows("y", k, rows)
        moves = []
        for n, (src_attn, src_ffn, to_a, to_b) in enumerate(
            ((local_attn, local_ffn, packed_a[k], packed_b[k]), (anchor_attn, anchor_ffn, base_a[k], base_b[k]))
        ):
            moves += [
                pltpu.make_async_copy(src_attn.at[at_a, :], to_a.at[:, pl.ds(0, attn)], sems.at[k, n, 0]),
                pltpu.make_async_copy(src_ffn.at[at_a, left], to_a.at[:, pl.ds(attn, cut)], sems.at[k, n, 1]),
                pltpu.make_async_copy(src_ffn.at[at_b, rest], to_b, sems.at[k, n, 2]),
            ]
        return moves

    order = (1, 3, 2, 0)
    moves = {k: fill(k) for k in order}
    for k in order:
        for move in moves[k]:
            move.start()
    sums = jnp.zeros((rows, 128), jnp.float32)
    for k in order:
        for move in moves[k]:
            move.wait()
        for local, base in ((packed_a[k], base_a[k]), (packed_b[k], base_b[k])):

            def step(i, acc, local=local, base=base):
                at = pl.ds(pl.multiple_of(i * 128, 128), 128)
                delta = local[:, at] - base[:, at]
                return acc + delta * delta

            sums = lax.fori_loop(0, local.shape[1] // 128, step, sums, unroll=4)
    total[...] = jnp.full(total.shape, jnp.sum(sums))


def pack(anchor_attn, anchor_ffn, local_attn, local_ffn):
    attn, ffn = local_attn.shape[1], local_ffn.shape[1]
    cut = (attn + ffn) // 7 * 3 - attn
    rows = local_attn.shape[0] // SIDE
    wide, narrow = (rows, attn + cut), (rows, ffn - cut)
    shapes = [wide] * SIDE + [narrow] * SIDE + [wide, narrow, (8, 128)]
    size = local_attn.size + local_ffn.size
    out = pl.pallas_call(
        functools.partial(pack_kernel, cut, rows, attn),
        name="pack",
        out_shape=[pltpu.VMEM(shape, jnp.float32) for shape in shapes],
        in_specs=[HBM] * 4,
        out_specs=[VMEM] * len(shapes),
        scratch_shapes=[
            pltpu.VMEM((SIDE - 1, *wide), jnp.float32),
            pltpu.VMEM((SIDE - 1, *narrow), jnp.float32),
            pltpu.SemaphoreType.DMA((SIDE, 2, 3)),
        ],
        compiler_params=PARAMS,
        cost_estimate=cost_of(3 * size, 16 * size),
    )(*held([anchor_attn, anchor_ffn, local_attn, local_ffn], pltpu.HBM))
    return out[:SIDE], out[SIDE : 2 * SIDE], *out[2 * SIDE :]


def weigh_kernel(axis, rows, pieces, *refs):
    blocks, squares, anchor, outs = refs[:SIDE], refs[SIDE : 2 * SIDE], refs[2 * SIDE], refs[-pieces:]
    weights = [jnp.minimum(jnp.float32(1.0), 1.0 / jnp.sqrt(s[:1, :1])) for s in squares]
    for k, out in enumerate(outs):
        at_rows = block_rows(axis, k, rows) if len(outs) > 1 else slice(None)

        def step(i, carry, at_rows=at_rows, out=out):
            at = pl.ds(pl.multiple_of(i * 128, 128), 128)
            base = anchor[at_rows, at]
            t = [w * (b[at_rows, at] - base) for w, b in zip(weights, blocks, strict=True)]
            out[:, at] = (t[0] + t[2]) + (t[1] + t[3])
            return carry

        lax.fori_loop(0, out.shape[1] // 128, step, 0, unroll=4)


def weigh(blocks, squares, anchor, axis, pieces, after=()):
    rows = anchor.shape[0] // pieces
    return pl.pallas_call(
        functools.partial(weigh_kernel, axis, rows, pieces),
        name="weigh",
        out_shape=[pltpu.VMEM((rows, anchor.shape[1]), anchor.dtype)] * pieces,
        in_specs=[VMEM] * (2 * SIDE + 1 + len(after)),
        out_specs=[VMEM] * pieces,
        compiler_params=PARAMS,
        cost_estimate=cost_of(11 * anchor.size, 24 * anchor.size),
    )(*held([*blocks, *squares, anchor, *after]))


def mean_kernel(*refs):
    blocks, out = refs[:SIDE], refs[SIDE]

    def step(i, carry):
        at = pl.ds(pl.multiple_of(i * 128, 128), 128)
        t = [b[:, at] for b in blocks]
        out[:, at] = ((t[0] + t[2]) + (t[1] + t[3])) * jnp.float32(1.0 / (SIDE * SIDE))
        return carry

    lax.fori_loop(0, out.shape[1] // 128, step, 0, unroll=4)


def mean(blocks):
    return pl.pallas_call(
        mean_kernel,
        name="mean",
        out_shape=pltpu.VMEM(blocks[0].shape, blocks[0].dtype),
        in_specs=[VMEM] * SIDE,
        out_specs=VMEM,
        compiler_params=PARAMS,
        cost_estimate=cost_of(4 * blocks[0].size, 20 * blocks[0].size),
    )(*held(blocks))


def join_kernel(axis, *refs):
    blocks, out = refs[:SIDE], refs[SIDE]
    rows = blocks[0].shape[0]
    for k, block in enumerate(blocks):
        at_rows = block_rows(axis, -k, rows)

        def step(i, carry, at_rows=at_rows, block=block):
            at = pl.ds(pl.multiple_of(i * 256, 256), 256)
            out[at_rows, at] = block[:, at]
            return carry

        lax.fori_loop(0, block.shape[1] // 256, step, 0)


def join(blocks, axis):
    rows, width = blocks[0].shape
    return pl.pallas_call(
        functools.partial(join_kernel, axis),
        name="join",
        out_shape=pltpu.VMEM((SIDE * rows, width), blocks[0].dtype),
        in_specs=[VMEM] * SIDE,
        out_specs=VMEM,
        compiler_params=PARAMS,
        cost_estimate=cost_of(rows * width, 32 * rows * width),
    )(*held(blocks))


def run(moves):
    for move in moves:
        move.start()
    for move in moves:
        move.wait()


def place_a_kernel(cut, rows, attn, *refs):
    blocks, (outer_attn, outer_ffn, sems) = refs[:SIDE], refs[SIDE:]
    moves = []
    for k in RING:
        at = block_rows("x", -k, rows)
        moves += [
            pltpu.make_async_copy(blocks[k].at[:, pl.ds(0, attn)], outer_attn.at[at, :], sems.at[k, 0]),
            pltpu.make_async_copy(blocks[k].at[:, pl.ds(attn, cut)], outer_ffn.at[at, pl.ds(0, cut)], sems.at[k, 1]),
        ]
    run(moves)


def place_b_kernel(cut, rows, *refs):
    blocks, (_, outer_ffn, sems) = refs[:SIDE], refs[SIDE:]
    columns = pl.ds(cut, outer_ffn.shape[1] - cut)
    run([
        pltpu.make_async_copy(blocks[k], outer_ffn.at[block_rows("y", -k, rows), columns], sems.at[k])
        for k in RING
    ])


def place(blocks_a, blocks_b, attn):
    rows, cut = blocks_a[0].shape[0], blocks_a[0].shape[1] - attn
    outer_attn = jax.ShapeDtypeStruct((SIDE * rows, attn), jnp.float32)
    outer_ffn = jax.ShapeDtypeStruct((SIDE * rows, cut + blocks_b[0].shape[1]), jnp.float32)
    placed_attn, placed_ffn = pl.pallas_call(
        functools.partial(place_a_kernel, cut, rows, attn),
        name="place_a",
        out_shape=[outer_attn, outer_ffn],
        in_specs=[VMEM] * SIDE,
        out_specs=[HBM] * 2,
        scratch_shapes=[pltpu.SemaphoreType.DMA((SIDE, 2))],
        compiler_params=PARAMS,
        cost_estimate=cost_of(0, 32 * blocks_a[0].size),
    )(*held(blocks_a))
    placed_ffn = pl.pallas_call(
        functools.partial(place_b_kernel, cut, rows),
        name="place_b",
        out_shape=outer_ffn,
        in_specs=[VMEM] * SIDE + [HBM],
        out_specs=HBM,
        scratch_shapes=[pltpu.SemaphoreType.DMA((SIDE,))],
        input_output_aliases={SIDE: 0},
        compiler_params=PARAMS,
        cost_estimate=cost_of(0, 32 * blocks_b[0].size),
    )(*held(blocks_b), *held([placed_ffn], pltpu.HBM))
    return placed_attn, placed_ffn


def sent(blocks, axis):
    received = {0: blocks[0]}
    for k in (1, 3, 2):
        received[k] = shifted(blocks[k], axis, k)
    return [received[k] for k in RING]


def total_over_shard(value):
    pair, near = (1, 0), (1, 0, 3, 2, 5, 4, 7, 6)
    other = paired(value, "core", pair)
    beside = paired(value, "z", near)
    both = [(2 * z + c, 2 * near[z] + pair[c]) for z in range(len(near)) for c in pair]
    across = lax.ppermute(value, ("z", "core"), both)
    value = (value + other) + (beside + across)
    value = value + paired(value, "z", (2, 3, 0, 1, 6, 7, 4, 5))
    return value + paired(value, "z", (6, 7, 4, 5, 2, 3, 0, 1))


def averaged(anchor_attn, anchor_ffn, local_attn, local_ffn):
    attn = anchor_attn.shape[1]
    blocks_a, blocks_b, anchor_a, anchor_b, partial = pack(anchor_attn, anchor_ffn, local_attn[0], local_ffn[0])
    raw_a = sent(blocks_a, "x")
    raw_b = sent(blocks_b, "y")
    squares = [total_over_shard(partial)] * SIDE
    parts_b = weigh(raw_b, sent(squares, "y"), anchor_b, "x", SIDE)
    (sum_a,) = weigh(raw_a, sent(squares, "x"), anchor_a, "y", 1, parts_b[:1])
    mean_b = mean(sent(parts_b, "x"))
    rows_a = mean(sent([sum_a] * SIDE, "y"))
    rows_b = join(sent([mean_b] * SIDE, "x"), "x")
    back_b = sent([rows_b] * SIDE, "y")
    return place(sent([rows_a] * SIDE, "x"), back_b, attn)


def solution(mesh):
    grid = Mesh(mesh.devices.reshape(SIDE, SIDE, -1, 2), ("y", "x", "z", "core"))
    rep, shard = ("y", "x"), ("z", "core")
    return jax.shard_map(
        averaged,
        mesh=grid,
        in_specs=(P(shard, None), P(shard, None), P(rep, shard, None), P(rep, shard, None)),
        out_specs=(P(shard, None), P(shard, None)),
        check_vma=False,
    )
```

```python
import functools

import jax
import jax.numpy as jnp
from jax import lax
from jax.experimental import pallas as pl
from jax.experimental.pallas import tpu as pltpu
from jax.sharding import Mesh, PartitionSpec as P


SIDE = 4
RING = range(SIDE)
VMEM = pl.BlockSpec(memory_space=pltpu.VMEM)
HBM = pl.BlockSpec(memory_space=pltpu.HBM)
PARAMS = pltpu.CompilerParams(vmem_limit_bytes=16 * 2**20)


def shifted(array, axis, step):
    return lax.ppermute(array, axis, [(i, (i + step) % SIDE) for i in RING])


def paired(value, axis, partner):
    return lax.ppermute(value, axis, list(enumerate(partner)))


def cost_of(flops, moved):
    return pl.CostEstimate(flops=flops, bytes_accessed=moved, transcendentals=0)


def held(arrays, space=pltpu.VMEM):
    return [pltpu.with_memory_space_constraint(a, space) for a in arrays]


def block_rows(axis, step, rows):
    block = lax.rem(lax.axis_index(axis) + (step + SIDE), SIDE)
    return pl.ds(pl.multiple_of(block * rows, rows), rows)


def pack_kernel(cut, rows, attn, anchor_attn, anchor_ffn, local_attn, local_ffn, *refs):
    packed_a, packed_b = refs[:SIDE], refs[SIDE : 2 * SIDE]
    first_a, first_b, total, later_a, later_b, sems = refs[2 * SIDE :]
    base_a = [first_a] + [later_a.at[k] for k in range(SIDE - 1)]
    base_b = [first_b] + [later_b.at[k] for k in range(SIDE - 1)]
    left, rest = pl.ds(0, cut), pl.ds(cut, local_ffn.shape[1] - cut)

    def fill(k):
        at_a, at_b = block_rows("x", k, rows), block_rows("y", k, rows)
        moves = []
        for n, (src_attn, src_ffn, to_a, to_b) in enumerate(
            ((local_attn, local_ffn, packed_a[k], packed_b[k]), (anchor_attn, anchor_ffn, base_a[k], base_b[k]))
        ):
            moves += [
                pltpu.make_async_copy(src_attn.at[at_a, :], to_a.at[:, pl.ds(0, attn)], sems.at[k, n, 0]),
                pltpu.make_async_copy(src_ffn.at[at_a, left], to_a.at[:, pl.ds(attn, cut)], sems.at[k, n, 1]),
                pltpu.make_async_copy(src_ffn.at[at_b, rest], to_b, sems.at[k, n, 2]),
            ]
        return moves

    order = (1, 3, 2, 0)
    moves = {k: fill(k) for k in order}
    for k in order:
        for move in moves[k]:
            move.start()
    sums = jnp.zeros((rows, 128), jnp.float32)
    for k in order:
        for move in moves[k]:
            move.wait()
        for local, base in ((packed_a[k], base_a[k]), (packed_b[k], base_b[k])):

            def step(i, acc, local=local, base=base):
                at = pl.ds(pl.multiple_of(i * 128, 128), 128)
                delta = local[:, at] - base[:, at]
                return acc + delta * delta

            sums = lax.fori_loop(0, local.shape[1] // 128, step, sums, unroll=4)
    total[...] = jnp.full(total.shape, jnp.sum(sums))


def pack(anchor_attn, anchor_ffn, local_attn, local_ffn):
    attn, ffn = local_attn.shape[1], local_ffn.shape[1]
    cut = (attn + ffn) // 2 - attn
    rows = local_attn.shape[0] // SIDE
    wide, narrow = (rows, attn + cut), (rows, ffn - cut)
    shapes = [wide] * SIDE + [narrow] * SIDE + [wide, narrow, (8, 128)]
    size = local_attn.size + local_ffn.size
    out = pl.pallas_call(
        functools.partial(pack_kernel, cut, rows, attn),
        name="pack",
        out_shape=[pltpu.VMEM(shape, jnp.float32) for shape in shapes],
        in_specs=[HBM] * 4,
        out_specs=[VMEM] * len(shapes),
        scratch_shapes=[
            pltpu.VMEM((SIDE - 1, *wide), jnp.float32),
            pltpu.VMEM((SIDE - 1, *narrow), jnp.float32),
            pltpu.SemaphoreType.DMA((SIDE, 2, 3)),
        ],
        compiler_params=PARAMS,
        cost_estimate=cost_of(3 * size, 16 * size),
    )(*held([anchor_attn, anchor_ffn, local_attn, local_ffn], pltpu.HBM))
    return out[:SIDE], out[SIDE : 2 * SIDE], *out[2 * SIDE :]


def weigh_kernel(axis, rows, pieces, *refs):
    blocks, squares, anchor, outs = refs[:SIDE], refs[SIDE : 2 * SIDE], refs[2 * SIDE], refs[-pieces:]
    weights = [jnp.minimum(jnp.float32(1.0), 1.0 / jnp.sqrt(s[:1, :1])) for s in squares]
    for k, out in enumerate(outs):
        at_rows = block_rows(axis, k, rows) if len(outs) > 1 else slice(None)

        def step(i, carry, at_rows=at_rows, out=out):
            at = pl.ds(pl.multiple_of(i * 128, 128), 128)
            base = anchor[at_rows, at]
            t = [w * (b[at_rows, at] - base) for w, b in zip(weights, blocks, strict=True)]
            out[:, at] = (t[0] + t[2]) + (t[1] + t[3])
            return carry

        lax.fori_loop(0, out.shape[1] // 128, step, 0, unroll=4)


def weigh(blocks, squares, anchor, axis, pieces, after=()):
    rows = anchor.shape[0] // pieces
    return pl.pallas_call(
        functools.partial(weigh_kernel, axis, rows, pieces),
        name="weigh",
        out_shape=[pltpu.VMEM((rows, anchor.shape[1]), anchor.dtype)] * pieces,
        in_specs=[VMEM] * (2 * SIDE + 1 + len(after)),
        out_specs=[VMEM] * pieces,
        compiler_params=PARAMS,
        cost_estimate=cost_of(11 * anchor.size, 24 * anchor.size),
    )(*held([*blocks, *squares, anchor, *after]))


def mean_kernel(*refs):
    blocks, out = refs[:SIDE], refs[SIDE]

    def step(i, carry):
        at = pl.ds(pl.multiple_of(i * 128, 128), 128)
        t = [b[:, at] for b in blocks]
        out[:, at] = ((t[0] + t[2]) + (t[1] + t[3])) * jnp.float32(1.0 / (SIDE * SIDE))
        return carry

    lax.fori_loop(0, out.shape[1] // 128, step, 0, unroll=4)


def mean(blocks):
    return pl.pallas_call(
        mean_kernel,
        name="mean",
        out_shape=pltpu.VMEM(blocks[0].shape, blocks[0].dtype),
        in_specs=[VMEM] * SIDE,
        out_specs=VMEM,
        compiler_params=PARAMS,
        cost_estimate=cost_of(4 * blocks[0].size, 20 * blocks[0].size),
    )(*held(blocks))


def join_kernel(axis, *refs):
    blocks, out = refs[:SIDE], refs[-1]
    rows = blocks[0].shape[0]
    for k, block in enumerate(blocks):
        at_rows = block_rows(axis, -k, rows)

        def step(i, carry, at_rows=at_rows, block=block):
            at = pl.ds(pl.multiple_of(i * 256, 256), 256)
            out[at_rows, at] = block[:, at]
            return carry

        lax.fori_loop(0, block.shape[1] // 256, step, 0)


def join(blocks, axis, after):
    rows, width = blocks[0].shape
    return pl.pallas_call(
        functools.partial(join_kernel, axis),
        name="join",
        out_shape=pltpu.VMEM((SIDE * rows, width), blocks[0].dtype),
        in_specs=[VMEM] * (SIDE + 1),
        out_specs=VMEM,
        compiler_params=PARAMS,
        cost_estimate=cost_of(rows * width, 32 * rows * width),
    )(*held([*blocks, after]))


def run(moves):
    for move in moves:
        move.start()
    for move in moves:
        move.wait()


def place_a_kernel(cut, rows, attn, *refs):
    blocks, (outer_attn, outer_ffn, sems) = refs[:SIDE], refs[SIDE:]
    moves = []
    for k in RING:
        at = block_rows("x", -k, rows)
        moves += [
            pltpu.make_async_copy(blocks[k].at[:, pl.ds(0, attn)], outer_attn.at[at, :], sems.at[k, 0]),
            pltpu.make_async_copy(blocks[k].at[:, pl.ds(attn, cut)], outer_ffn.at[at, pl.ds(0, cut)], sems.at[k, 1]),
        ]
    run(moves)


def place_b_kernel(cut, rows, *refs):
    blocks, (_, outer_ffn, sems) = refs[:SIDE], refs[SIDE:]
    columns = pl.ds(cut, outer_ffn.shape[1] - cut)
    run([
        pltpu.make_async_copy(blocks[k], outer_ffn.at[block_rows("y", -k, rows), columns], sems.at[k])
        for k in RING
    ])


def place(blocks_a, blocks_b, attn):
    rows, cut = blocks_a[0].shape[0], blocks_a[0].shape[1] - attn
    outer_attn = jax.ShapeDtypeStruct((SIDE * rows, attn), jnp.float32)
    outer_ffn = jax.ShapeDtypeStruct((SIDE * rows, cut + blocks_b[0].shape[1]), jnp.float32)
    placed_attn, placed_ffn = pl.pallas_call(
        functools.partial(place_a_kernel, cut, rows, attn),
        name="place_a",
        out_shape=[outer_attn, outer_ffn],
        in_specs=[VMEM] * SIDE,
        out_specs=[HBM] * 2,
        scratch_shapes=[pltpu.SemaphoreType.DMA((SIDE, 2))],
        compiler_params=PARAMS,
        cost_estimate=cost_of(0, 32 * blocks_a[0].size),
    )(*held(blocks_a))
    placed_ffn = pl.pallas_call(
        functools.partial(place_b_kernel, cut, rows),
        name="place_b",
        out_shape=outer_ffn,
        in_specs=[VMEM] * SIDE + [HBM],
        out_specs=HBM,
        scratch_shapes=[pltpu.SemaphoreType.DMA((SIDE,))],
        input_output_aliases={SIDE: 0},
        compiler_params=PARAMS,
        cost_estimate=cost_of(0, 32 * blocks_b[0].size),
    )(*held(blocks_b), *held([placed_ffn], pltpu.HBM))
    return placed_attn, placed_ffn


def sent(blocks, axis):
    received = {0: blocks[0]}
    for k in (1, 3, 2):
        received[k] = shifted(blocks[k], axis, k)
    return [received[k] for k in RING]


def total_over_shard(value):
    value = value + paired(value, "core", (1, 0))
    for partner in ((1, 0, 3, 2, 5, 4, 7, 6), (2, 3, 0, 1, 6, 7, 4, 5), (6, 7, 4, 5, 2, 3, 0, 1)):
        value = value + paired(value, "z", partner)
    return value


def averaged(anchor_attn, anchor_ffn, local_attn, local_ffn):
    attn = anchor_attn.shape[1]
    blocks_a, blocks_b, anchor_a, anchor_b, partial = pack(anchor_attn, anchor_ffn, local_attn[0], local_ffn[0])
    raw_a = sent(blocks_a, "x")
    raw_b = sent(blocks_b, "y")
    squares = [total_over_shard(partial)] * SIDE
    squares_a, squares_b = sent(squares, "x"), sent(squares, "y")
    (sum_a,) = weigh(raw_a, squares_a, anchor_a, "y", 1)
    parts_b = weigh(raw_b, squares_b, anchor_b, "x", SIDE, (sum_a,))
    mean_b = mean(sent(parts_b, "x"))
    rows_a = mean(sent([sum_a] * SIDE, "y"))
    rows_b = join(sent([mean_b] * SIDE, "x"), "x", rows_a)
    back_a = sent([rows_a] * SIDE, "x")
    return place(back_a, sent([rows_b] * SIDE, "y"), attn)


def solution(mesh):
    grid = Mesh(mesh.devices.reshape(SIDE, SIDE, -1, 2), ("y", "x", "z", "core"))
    rep, shard = ("y", "x"), ("z", "core")
    return jax.shard_map(
        averaged,
        mesh=grid,
        in_specs=(P(shard, None), P(shard, None), P(rep, shard, None), P(rep, shard, None)),
        out_specs=(P(shard, None), P(shard, None)),
        check_vma=False,
    )
```

```python
import functools

import jax
import jax.numpy as jnp
from jax import lax
from jax.experimental import pallas as pl
from jax.experimental.pallas import tpu as pltpu
from jax.sharding import Mesh, PartitionSpec as P


SIDE = 4
RING = range(SIDE)
VMEM = pl.BlockSpec(memory_space=pltpu.VMEM)
HBM = pl.BlockSpec(memory_space=pltpu.HBM)
PARAMS = pltpu.CompilerParams(vmem_limit_bytes=16 * 2**20)


def shifted(array, axis, step):
    return lax.ppermute(array, axis, [(i, (i + step) % SIDE) for i in RING])


def paired(value, axis, partner):
    return lax.ppermute(value, axis, list(enumerate(partner)))


def cost_of(flops, moved):
    return pl.CostEstimate(flops=flops, bytes_accessed=moved, transcendentals=0)


def held(arrays, space=pltpu.VMEM):
    return [pltpu.with_memory_space_constraint(a, space) for a in arrays]


def block_rows(axis, step, rows):
    block = lax.rem(lax.axis_index(axis) + (step + SIDE), SIDE)
    return pl.ds(pl.multiple_of(block * rows, rows), rows)


def pack_kernel(cut, rows, attn, anchor_attn, anchor_ffn, local_attn, local_ffn, *refs):
    packed_a, packed_b = refs[:SIDE], refs[SIDE : 2 * SIDE]
    first_a, first_b, total, later_a, later_b, sems = refs[2 * SIDE :]
    base_a = [first_a] + [later_a.at[k] for k in range(SIDE - 1)]
    base_b = [first_b] + [later_b.at[k] for k in range(SIDE - 1)]
    left, rest = pl.ds(0, cut), pl.ds(cut, local_ffn.shape[1] - cut)

    def fill(k):
        at_a, at_b = block_rows("x", k, rows), block_rows("y", k, rows)
        moves = []
        for n, (src_attn, src_ffn, to_a, to_b) in enumerate(
            ((local_attn, local_ffn, packed_a[k], packed_b[k]), (anchor_attn, anchor_ffn, base_a[k], base_b[k]))
        ):
            moves += [
                pltpu.make_async_copy(src_attn.at[at_a, :], to_a.at[:, pl.ds(0, attn)], sems.at[k, n, 0]),
                pltpu.make_async_copy(src_ffn.at[at_a, left], to_a.at[:, pl.ds(attn, cut)], sems.at[k, n, 1]),
                pltpu.make_async_copy(src_ffn.at[at_b, rest], to_b, sems.at[k, n, 2]),
            ]
        return moves

    order = (1, 3, 2, 0)
    moves = {k: fill(k) for k in order}
    for k in order:
        for move in moves[k]:
            move.start()
    sums = jnp.zeros((rows, 128), jnp.float32)
    for k in order:
        for move in moves[k]:
            move.wait()
        for local, base in ((packed_a[k], base_a[k]), (packed_b[k], base_b[k])):

            def step(i, acc, local=local, base=base):
                at = pl.ds(pl.multiple_of(i * 128, 128), 128)
                delta = local[:, at] - base[:, at]
                return acc + delta * delta

            sums = lax.fori_loop(0, local.shape[1] // 128, step, sums, unroll=2)
    total[...] = jnp.full(total.shape, jnp.sum(sums))


def pack(anchor_attn, anchor_ffn, local_attn, local_ffn):
    attn, ffn = local_attn.shape[1], local_ffn.shape[1]
    cut = (attn + ffn) // 28 * 13 - attn
    rows = local_attn.shape[0] // SIDE
    wide, narrow = (rows, attn + cut), (rows, ffn - cut)
    shapes = [wide] * SIDE + [narrow] * SIDE + [wide, narrow, (8, 128)]
    size = local_attn.size + local_ffn.size
    out = pl.pallas_call(
        functools.partial(pack_kernel, cut, rows, attn),
        name="pack",
        out_shape=[pltpu.VMEM(shape, jnp.float32) for shape in shapes],
        in_specs=[HBM] * 4,
        out_specs=[VMEM] * len(shapes),
        scratch_shapes=[
            pltpu.VMEM((SIDE - 1, *wide), jnp.float32),
            pltpu.VMEM((SIDE - 1, *narrow), jnp.float32),
            pltpu.SemaphoreType.DMA((SIDE, 2, 3)),
        ],
        compiler_params=PARAMS,
        cost_estimate=cost_of(3 * size, 16 * size),
    )(*held([anchor_attn, anchor_ffn, local_attn, local_ffn], pltpu.HBM))
    return out[:SIDE], out[SIDE : 2 * SIDE], *out[2 * SIDE :]


def weigh_kernel(axis, rows, pieces, *refs):
    blocks, squares, anchor, outs = refs[:SIDE], refs[SIDE : 2 * SIDE], refs[2 * SIDE], refs[-pieces:]
    weights = [jnp.minimum(jnp.float32(1.0), 1.0 / jnp.sqrt(s[:1, :1])) for s in squares]
    for k, out in enumerate(outs):
        at_rows = block_rows(axis, k, rows) if len(outs) > 1 else slice(None)

        def step(i, carry, at_rows=at_rows, out=out):
            at = pl.ds(pl.multiple_of(i * 128, 128), 128)
            base = anchor[at_rows, at]
            t = [w * (b[at_rows, at] - base) for w, b in zip(weights, blocks, strict=True)]
            out[:, at] = (t[0] + t[2]) + (t[1] + t[3])
            return carry

        lax.fori_loop(0, out.shape[1] // 128, step, 0, unroll=2 if len(outs) == 1 else 6)


def weigh(blocks, squares, anchor, axis, pieces, after=()):
    rows = anchor.shape[0] // pieces
    return pl.pallas_call(
        functools.partial(weigh_kernel, axis, rows, pieces),
        name="weigh",
        out_shape=[pltpu.VMEM((rows, anchor.shape[1]), anchor.dtype)] * pieces,
        in_specs=[VMEM] * (2 * SIDE + 1 + len(after)),
        out_specs=[VMEM] * pieces,
        compiler_params=PARAMS,
        cost_estimate=cost_of(11 * anchor.size, 24 * anchor.size),
    )(*held([*blocks, *squares, anchor, *after]))


def mean_kernel(*refs):
    blocks, out = refs[:SIDE], refs[SIDE]

    def step(i, carry):
        at = pl.ds(pl.multiple_of(i * 128, 128), 128)
        t = [b[:, at] for b in blocks]
        out[:, at] = ((t[0] + t[2]) + (t[1] + t[3])) * jnp.float32(1.0 / (SIDE * SIDE))
        return carry

    lax.fori_loop(0, out.shape[1] // 128, step, 0, unroll=2)


def mean(blocks):
    return pl.pallas_call(
        mean_kernel,
        name="mean",
        out_shape=pltpu.VMEM(blocks[0].shape, blocks[0].dtype),
        in_specs=[VMEM] * SIDE,
        out_specs=VMEM,
        compiler_params=PARAMS,
        cost_estimate=cost_of(4 * blocks[0].size, 20 * blocks[0].size),
    )(*held(blocks))


def join_kernel(axis, *refs):
    blocks, out = refs[:SIDE], refs[-1]
    rows = blocks[0].shape[0]
    for k, block in enumerate(blocks):
        at_rows = block_rows(axis, -k, rows)

        def step(i, carry, at_rows=at_rows, block=block):
            at = pl.ds(pl.multiple_of(i * 256, 256), 256)
            out[at_rows, at] = block[:, at]
            return carry

        lax.fori_loop(0, block.shape[1] // 256, step, 0)


def join(blocks, axis, after):
    rows, width = blocks[0].shape
    return pl.pallas_call(
        functools.partial(join_kernel, axis),
        name="join",
        out_shape=pltpu.VMEM((SIDE * rows, width), blocks[0].dtype),
        in_specs=[VMEM] * (SIDE + 1),
        out_specs=VMEM,
        compiler_params=PARAMS,
        cost_estimate=cost_of(rows * width, 32 * rows * width),
    )(*held([*blocks, after]))


def run(moves):
    for move in moves:
        move.start()
    for move in moves:
        move.wait()


def place_a_kernel(cut, rows, attn, *refs):
    blocks, (outer_attn, outer_ffn, sems) = refs[:SIDE], refs[SIDE:]
    moves = []
    for k in RING:
        at = block_rows("x", -k, rows)
        moves += [
            pltpu.make_async_copy(blocks[k].at[:, pl.ds(0, attn)], outer_attn.at[at, :], sems.at[k, 0]),
            pltpu.make_async_copy(blocks[k].at[:, pl.ds(attn, cut)], outer_ffn.at[at, pl.ds(0, cut)], sems.at[k, 1]),
        ]
    run(moves)


def place_b_kernel(cut, rows, *refs):
    blocks, (_, outer_ffn, sems) = refs[:SIDE], refs[SIDE:]
    columns = pl.ds(cut, outer_ffn.shape[1] - cut)
    run([
        pltpu.make_async_copy(blocks[k], outer_ffn.at[block_rows("y", -k, rows), columns], sems.at[k])
        for k in RING
    ])


def place(blocks_a, blocks_b, attn):
    rows, cut = blocks_a[0].shape[0], blocks_a[0].shape[1] - attn
    outer_attn = jax.ShapeDtypeStruct((SIDE * rows, attn), jnp.float32)
    outer_ffn = jax.ShapeDtypeStruct((SIDE * rows, cut + blocks_b[0].shape[1]), jnp.float32)
    placed_attn, placed_ffn = pl.pallas_call(
        functools.partial(place_a_kernel, cut, rows, attn),
        name="place_a",
        out_shape=[outer_attn, outer_ffn],
        in_specs=[VMEM] * SIDE,
        out_specs=[HBM] * 2,
        scratch_shapes=[pltpu.SemaphoreType.DMA((SIDE, 2))],
        compiler_params=PARAMS,
        cost_estimate=cost_of(0, 32 * blocks_a[0].size),
    )(*held(blocks_a))
    placed_ffn = pl.pallas_call(
        functools.partial(place_b_kernel, cut, rows),
        name="place_b",
        out_shape=outer_ffn,
        in_specs=[VMEM] * SIDE + [HBM],
        out_specs=HBM,
        scratch_shapes=[pltpu.SemaphoreType.DMA((SIDE,))],
        input_output_aliases={SIDE: 0},
        compiler_params=PARAMS,
        cost_estimate=cost_of(0, 32 * blocks_b[0].size),
    )(*held(blocks_b), *held([placed_ffn], pltpu.HBM))
    return placed_attn, placed_ffn


def sent(blocks, axis):
    received = {0: blocks[0]}
    for k in (1, 3, 2):
        received[k] = shifted(blocks[k], axis, k)
    return [received[k] for k in RING]


def total_over_shard(value):
    value = value + paired(value, "core", (1, 0))
    for partner in ((1, 0, 3, 2, 5, 4, 7, 6), (2, 3, 0, 1, 6, 7, 4, 5), (6, 7, 4, 5, 2, 3, 0, 1)):
        value = value + paired(value, "z", partner)
    return value


def averaged(anchor_attn, anchor_ffn, local_attn, local_ffn):
    attn = anchor_attn.shape[1]
    blocks_a, blocks_b, anchor_a, anchor_b, partial = pack(anchor_attn, anchor_ffn, local_attn[0], local_ffn[0])
    raw_a = sent(blocks_a, "x")
    raw_b = sent(blocks_b, "y")
    squares = [total_over_shard(partial)] * SIDE
    squares_a, squares_b = sent(squares, "x"), sent(squares, "y")
    (sum_a,) = weigh(raw_a, squares_a, anchor_a, "y", 1)
    parts_b = weigh(raw_b, squares_b, anchor_b, "x", SIDE, (sum_a,))
    mean_b = mean(sent(parts_b, "x"))
    rows_a = mean(sent([sum_a] * SIDE, "y"))
    rows_b = join(sent([mean_b] * SIDE, "x"), "x", rows_a)
    back_a = sent([rows_a] * SIDE, "x")
    return place(back_a, sent([rows_b] * SIDE, "y"), attn)


def solution(mesh):
    grid = Mesh(mesh.devices.reshape(SIDE, SIDE, -1, 2), ("y", "x", "z", "core"))
    rep, shard = ("y", "x"), ("z", "core")
    return jax.shard_map(
        averaged,
        mesh=grid,
        in_specs=(P(shard, None), P(shard, None), P(rep, shard, None), P(rep, shard, None)),
        out_specs=(P(shard, None), P(shard, None)),
        check_vma=False,
    )
```
